128 devices in a mesh: seq: 16 (over z_hi, y, core), tensor: 8 (over z_lo, x).
Axes of the slice: x: 4, y: 4, z: 4 (z_hi: 2, z_lo: 2; z = z_hi * 2 + z_lo), core: 2. Of those that a mesh axis runs over, the one named last changes fastest.
Arguments:
- tokens: bfloat16 [11520, 1536], P('seq'), may hold values from -6 to 6
- norm_gain: float32 [1536], replicated, may hold values from 0.1 to 1.9
- w_qkv: bfloat16 [1536, 3, 1536], P(None, None, 'tensor'), may hold values from -8 to 8
- w_out: bfloat16 [1536, 1536], P('tensor'), may hold values from -0.15625 to 0.15625
- post_gain: float32 [1536], replicated, may hold values from 0.1 to 1.9
- w_up: bfloat16 [1536, 6144], P(None, 'tensor'), may hold values from -0.15625 to 0.15625
- w_down: bfloat16 [6144, 1536], P('tensor'), may hold values from -0.078125 to 0.078125
Outputs:
- layer_out: bfloat16 [11520, 1536], P('seq')
The draws below stay inside these ranges and needn't reach their ends.
All inputs are finite; a program needn't handle non-finite values.
Results may differ from the reference program's by a relative error of at most 0.015.
Values may be sent and summed in bfloat16 or wider, within the bound.
No kernel may reach another device: no remote copies, remote signals or barrier semaphores. Data moves between devices by JAX's collectives and lax.ppermute only.
A program may use at most 128 MiB of HBM per device.

```python
import math
import jax
import jax.numpy as jnp
from jax import lax

D = 1536
HEADS = 32
HD = 48
FF = 6144
TOK_DEV = 720
TOKENS = 11520
N_TENSOR = 8


def draw_w_qkv(key, part):
    base = jax.random.normal(key, (D, 3, HEADS * HD), jnp.float32) * D ** (-0.5)
    levels = jax.random.uniform(jax.random.fold_in(key, 3), (HEADS,), jnp.float32, math.log(1.5), math.log(3.5))
    sharpness = jnp.repeat(jnp.exp(levels), HD)
    query = base[:, 0, :] * sharpness[None, :]
    stacked = jnp.stack([query, base[:, 1, :], base[:, 2, :]], axis=1)
    return jnp.clip(stacked, -8.0, 8.0).astype(jnp.bfloat16)


def level_of(stream_key, shape, cuts, least, top_value):
    def one(dim, parts):
        steps = jax.random.uniform(jax.random.fold_in(jax.random.fold_in(stream_key, 6), dim), (parts,), jnp.float32, least / len(cuts), top_value / len(cuts))
        return jnp.repeat(jnp.exp(steps), shape[dim] // parts).reshape((-1,) + (1,) * (len(shape) - dim - 1))

    level = one(*cuts[0])
    for cut in cuts[1:]:
        level = level * one(*cut)
    return level


def scatter_about(rng, extent, scale, bound, split=(), dtype=jnp.bfloat16):
    loudness = level_of(rng, extent, split, -0.22, 0.18) if split else 1.0
    array = jax.random.normal(rng, extent, jnp.float32) * scale * loudness
    return jnp.minimum(jnp.maximum(array, -bound), bound).astype(dtype)


def setup_inputs(seed: int = 0) -> dict:
    key_list = jax.random.split(jax.random.key(seed), 8)
    return {
        "tokens": scatter_about(key_list[0], (TOKENS, D), 1.0, 6.0, ((0, 16),)),
        "norm_gain": jnp.clip(1.0 + 0.18 * jax.random.normal(key_list[1], (D,), jnp.float32), 0.1, 1.9),
        "w_qkv": draw_w_qkv(jax.random.fold_in(key_list[7], 71), 0),
        "w_out": scatter_about(key_list[3], (HEADS * HD, D), (HEADS * HD) ** -0.5, 0.15625, ((0, 8),)),
        "post_gain": jnp.clip(1.0 + 0.18 * jax.random.normal(key_list[4], (D,), jnp.float32), 0.1, 1.9),
        "w_up": scatter_about(key_list[5], (D, FF), D ** -0.5, 0.15625, ((1, 8),)),
        "w_down": scatter_about(key_list[6], (FF, D), FF ** -0.5, 0.078125, ((0, 8),)),
    }


def layer_norm(values, gain):
    mean = lax.optimization_barrier(jnp.mean(values, axis=-1, keepdims=True))
    centred = values - mean
    var = lax.optimization_barrier(jnp.mean(centred * centred, axis=-1, keepdims=True))
    return centred * lax.rsqrt(var + 1e-05) * gain

def one_head(operands):
    query, key, value = operands
    scale = 1.0 / HD ** 0.5

    def block(query_block):
        scores = jnp.dot(query_block, key.T, preferred_element_type=jnp.float32) * scale
        peak = lax.optimization_barrier(jnp.max(scores, axis=-1, keepdims=True))
        weights = jnp.exp(scores - peak)
        total = lax.optimization_barrier(jnp.sum(weights, axis=-1, keepdims=True))
        return jnp.dot(weights.astype(jnp.bfloat16), value, preferred_element_type=jnp.float32) / total
    blocks = query.reshape(TOKENS // TOK_DEV, TOK_DEV, HD)
    return lax.map(block, blocks).reshape(TOKENS, HD)

def grouped_sum(left, right):
    width = left.shape[1] // N_TENSOR
    result = jnp.zeros((left.shape[0], right.shape[1]), jnp.float32)
    for group in range(N_TENSOR):
        term = jnp.dot(left[:, group * width:(group + 1) * width], right[group * width:(group + 1) * width], preferred_element_type=jnp.float32)
        term = lax.optimization_barrier(term.astype(jnp.bfloat16))
        result = result + term.astype(jnp.float32)
    return result

def reference(tokens, norm_gain, w_qkv, w_out, post_gain, w_up, w_down):
    base = tokens.astype(jnp.float32)
    normed = layer_norm(base, norm_gain).astype(jnp.bfloat16)
    qkv = jnp.dot(normed, w_qkv.reshape(D, 3 * HEADS * HD), preferred_element_type=jnp.float32).astype(jnp.bfloat16)
    qkv = qkv.reshape(TOKENS, 3, HEADS, HD)
    query = jnp.transpose(qkv[:, 0], (1, 0, 2))
    key = jnp.transpose(qkv[:, 1], (1, 0, 2))
    value = jnp.transpose(qkv[:, 2], (1, 0, 2))
    heads = lax.map(one_head, (query, key, value))
    attended = jnp.transpose(heads, (1, 0, 2)).reshape(TOKENS, HEADS * HD).astype(jnp.bfloat16)
    mixed = base + grouped_sum(attended, w_out)
    post = layer_norm(mixed, post_gain).astype(jnp.bfloat16)
    hidden = jax.nn.gelu(jnp.dot(post, w_up, preferred_element_type=jnp.float32), approximate=True).astype(jnp.bfloat16)
    return (mixed + grouped_sum(hidden, w_down)).astype(jnp.bfloat16)
```

```python
import functools

import jax
import jax.numpy as jnp
from jax import lax
from jax.experimental import pallas as pl
from jax.experimental.pallas import tpu as pltpu
from jax.sharding import Mesh
from jax.sharding import PartitionSpec as P


HD = 48
TOK = 720
PAD = 768
SLAB = 96
QW = 256
LOG2E = 1.4426950408889634
SAFE = 90.0 * 90.0
BF = jnp.bfloat16
F32 = jnp.float32


def layer_norm(values, gain):
    mean = jnp.mean(values, axis=-1, keepdims=True)
    centred = values - mean
    var = jnp.mean(centred * centred, axis=-1, keepdims=True)
    return centred * lax.rsqrt(var + 1e-05) * gain


def swap(x, axis, size, s):
    return lax.ppermute(x, axis, [(i, i ^ s) for i in range(size)])


def pick(x, index, axis=0):
    return lax.dynamic_index_in_dim(x, index, axis, keepdims=False)


def attend_kernel(*refs, first, last):
    if first:
        q_ref, a_ref, b_ref, o_ref, m_ref, keys, kmax = refs
    else:
        q_ref, a_ref, b_ref, acc_ref, min_ref, o_ref, keys, kmax = refs
    halves = (a_ref, b_ref)

    @pl.when(pl.program_id(0) == 0)
    def _():
        most = jnp.zeros((1, TOK), F32)
        for h, ref in enumerate(halves):
            for s in range(4):
                kt = ref[s, 0, :, :TOK].astype(F32)
                most = jnp.maximum(most, jnp.sum(kt * kt, axis=0, keepdims=True))
                keys[h * 4 + s] = kt.T.astype(BF)
        kmax[0] = jnp.max(most)

    qf = q_ref[...].astype(F32)
    norm = jnp.max(jnp.sum(qf * qf, axis=0, keepdims=True)) * kmax[0]
    safe = norm <= SAFE
    if not first:
        safe = jnp.logical_and(safe, jnp.max(jnp.abs(min_ref[...])) == 0.0)
    ones = jnp.ones((16, TOK), BF)

    def values(h, s):
        return jnp.concatenate([halves[h][s, 1, :, :TOK], ones], 0)

    def finish(j, acc, m):
        if last:
            o_ref[:, pl.ds(j, QW)] = (acc[:HD] / acc[HD : HD + 1]).astype(BF)
        else:
            o_ref[:, pl.ds(j, QW)] = acc
            m_ref[:, pl.ds(j, QW)] = m

    @pl.when(safe)
    def _():
        for j in range(0, PAD, QW):
            qt = q_ref[:, pl.ds(j, QW)]
            acc = jnp.zeros((64, QW), F32) if first else acc_ref[:, pl.ds(j, QW)]
            for h in range(2):
                for s in range(4):
                    scores = jnp.dot(keys[h * 4 + s], qt, preferred_element_type=F32)
                    weights = jnp.exp2(scores).astype(BF)
                    acc = acc + jnp.dot(values(h, s), weights, preferred_element_type=F32)
            finish(j, acc, jnp.zeros((1, QW), F32))

    @pl.when(jnp.logical_not(safe))
    def _():
        def column(c, _):
            j = pl.multiple_of(c * QW, QW)
            qt = q_ref[:, pl.ds(j, QW)]
            if first:
                state = (jnp.full((1, QW), -1e30, F32), jnp.zeros((64, QW), F32))
            else:
                state = (min_ref[:, pl.ds(j, QW)], acc_ref[:, pl.ds(j, QW)])
            for h in range(2):

                def block(s, st, h=h):
                    m, acc = st
                    scores = jnp.dot(keys[h * 4 + s], qt, preferred_element_type=F32)
                    fresh = jnp.maximum(m, jnp.max(scores, axis=0, keepdims=True))
                    weights = jnp.exp2(scores - fresh).astype(BF)
                    acc = acc * jnp.exp2(m - fresh)
                    return fresh, acc + jnp.dot(values(h, s), weights, preferred_element_type=F32)

                state = lax.fori_loop(0, 4, block, state)
            finish(j, state[1], state[0])
            return 0

        lax.fori_loop(0, PAD // QW, column, 0)


def attend(q, kv_a, kv_b, carry=None):
    first = carry is None
    row = lambda *shape: pl.BlockSpec((None, *shape), lambda i: (i, 0, 0))
    whole = pl.BlockSpec((4, 2, HD, PAD), lambda i: (0, 0, 0, 0))
    ins = [row(HD, PAD), whole, whole]
    if first:
        out_shape = (
            jax.ShapeDtypeStruct((4, 64, PAD), F32),
            jax.ShapeDtypeStruct((4, 1, PAD), F32),
        )
        out_specs = (row(64, PAD), row(1, PAD))
    else:
        ins += [row(64, PAD), row(1, PAD)]
        out_shape = jax.ShapeDtypeStruct((4, HD, PAD), BF)
        out_specs = row(HD, PAD)
    pairs = 4 * PAD * 8 * TOK
    return pl.pallas_call(
        functools.partial(attend_kernel, first=first, last=not first),
        out_shape=out_shape,
        grid=(4,),
        in_specs=ins,
        out_specs=out_specs,
        scratch_shapes=[pltpu.VMEM((8, TOK, HD), BF), pltpu.SMEM((1,), F32)],
        compiler_params=pltpu.CompilerParams(vmem_limit_bytes=40 * 2**20),
        cost_estimate=pl.CostEstimate(
            flops=pairs * 8 * HD, transcendentals=pairs, bytes_accessed=4 * 2**20
        ),
        name="attend_a" if first else "attend_b",
    )(q, kv_a, kv_b, *(() if first else carry))


def place_kernel(t_ref, *refs):
    slabs, o_ref = refs[:8], refs[8]
    t = t_ref[0]
    for s in range(8):
        where = t ^ s

        @pl.when(where < 7)
        def _(s=s, where=where):
            o_ref[pl.ds(pl.multiple_of(where * SLAB, 16), SLAB), :] = slabs[s][...]

        @pl.when(where == 7)
        def _(s=s):
            o_ref[7 * SLAB : TOK, :] = slabs[s][: TOK - 7 * SLAB, :]


def place(t, slabs):
    vmem = pl.BlockSpec(memory_space=pltpu.VMEM)
    return pl.pallas_call(
        place_kernel,
        out_shape=jax.ShapeDtypeStruct((TOK, slabs[0].shape[1]), BF),
        in_specs=[pl.BlockSpec(memory_space=pltpu.SMEM)] + [vmem] * 8,
        out_specs=vmem,
        name="place",
    )(t.reshape(1), *slabs)


def gelu(x):
    return jax.nn.gelu(x, approximate=True).astype(BF)


def dot(a, b):
    return jnp.dot(a, b, preferred_element_type=F32)


def per_device(tokens, norm_gain, w_qkv, w_out, post_gain, w_up, w_down):
    y, core = lax.axis_index("y"), lax.axis_index("core")
    zl, x = lax.axis_index("zl"), lax.axis_index("x")
    width = tokens.shape[1]

    half = w_up.shape[1] // 2
    up_half = lax.dynamic_slice_in_dim(w_up, core * half, half, 1)
    down_half = lax.dynamic_slice_in_dim(w_down, core * half, half, 0)
    up_a = swap(up_half, "zl", 2, 1)
    down_a = swap(down_half, "zl", 2, 1)

    padded = jnp.pad(tokens, ((0, PAD - TOK), (0, 0)))
    normed = layer_norm(padded.astype(F32), norm_gain).astype(BF)
    qkv = lax.dot_general(
        w_qkv.reshape(width, -1), normed, (((0,), (1,)), ((), ())), preferred_element_type=F32
    )
    span = 4 * HD
    qkv = jnp.concatenate([qkv[:span] * (LOG2E / HD**0.5), qkv[span:]], 0).astype(BF)
    qkv = qkv.reshape(3, 4, HD, PAD)

    mine = [pick(qkv, y ^ s, 1) for s in range(4)]
    got = [mine[0]] + [swap(mine[s], "y", 4, s) for s in range(1, 4)]
    q = jnp.stack([g[0] for g in got])
    kv = jnp.stack([g[1:] for g in got])
    kv_z = swap(kv, "zh", 2, 1)
    kv_c = swap(kv, "core", 2, 1)
    kv_zc = swap(kv_z, "core", 2, 1)
    part = attend(q, kv, kv_c)
    out_a = swap(w_out, "zl", 2, 1)
    up_b = swap(up_a, "core", 2, 1)
    down_b = swap(down_a, "core", 2, 1)
    heads = attend(q, kv_z, kv_zc, part)

    back = [heads[0]] + [swap(heads[s], "y", 4, s) for s in range(1, 4)]
    att = jnp.concatenate(back, 0)
    keep = lax.dynamic_slice_in_dim(att, zl * (PAD // 2), PAD // 2, 1)
    give = lax.dynamic_slice_in_dim(att, (1 - zl) * (PAD // 2), PAD // 2, 1)
    other = swap(give, "zl", 2, 1)

    def ordered(w):
        w = w.reshape(4, HD, width)
        return [pick(w, y ^ s) for s in range(4)]

    rows = jnp.concatenate(ordered(w_out) + ordered(out_a), 0)
    both = jnp.concatenate([keep, other], 0)
    term = lax.dot_general(both, rows, (((0,), (0,)), ((), ())), preferred_element_type=F32)
    term = term.astype(BF).reshape(4, SLAB, width)
    terms = [pick(term, x)] + [swap(pick(term, x ^ s), "x", 4, s) for s in range(1, 4)]
    base = lax.dynamic_slice_in_dim(padded, (zl * 4 + x) * SLAB, SLAB, 0).astype(F32)
    mixed = base + sum(t.astype(F32) for t in terms)

    post = layer_norm(mixed, post_gain).astype(BF)
    posts = jnp.concatenate([post] + [swap(post, "x", 4, s) for s in range(1, 4)], 0)
    down = dot(gelu(dot(posts, w_up)), w_down)
    down = down + dot(gelu(dot(posts, up_a)), down_a)
    down = down + dot(gelu(dot(posts, up_b)), down_b)
    down = down.astype(BF).reshape(4, SLAB, width)
    downs = [down[0]] + [swap(down[s], "x", 4, s) for s in range(1, 4)]
    final = (mixed + sum(d.astype(F32) for d in downs)).astype(BF)
    slabs = [final] + [swap(final, ("zl", "x"), 8, s) for s in range(1, 8)]
    return place(zl * 4 + x, slabs)


def solution(mesh):
    fine = Mesh(mesh.devices.reshape(2, 4, 2, 2, 4), ("zh", "y", "core", "zl", "x"))
    seq, ten = ("zh", "y", "core"), ("zl", "x")
    placed = (
        P(seq, None),
        P(),
        P(None, None, ten),
        P(ten, None),
        P(),
        P(None, ten),
        P(ten, None),
    )
    return jax.shard_map(
        per_device, mesh=fine, in_specs=placed, out_specs=P(seq, None), check_vma=False
    )
```

```python
import functools

import jax
import jax.numpy as jnp
from jax import lax
from jax.experimental import pallas as pl
from jax.experimental.pallas import tpu as pltpu
from jax.sharding import Mesh
from jax.sharding import PartitionSpec as P


HD = 48
D = 1536
TOK = 720
PAD = 768
QW = 512
ALL = 4 * PAD
CHUNKS = ((0, 256, 32), (256, 512, 64))
LOG2E = 1.4426950408889634
SAFE = 90.0 * 90.0
BF = jnp.bfloat16
F32 = jnp.float32
VMEM = pl.BlockSpec(memory_space=pltpu.VMEM)
SMEM = pl.BlockSpec(memory_space=pltpu.SMEM)
PAIR = 1
TENSOR = ("zl", "xh", "xl")
GROUP = (3, 4, 7)


def swap(x, axis, size, s):
    return lax.ppermute(x, axis, [(i, i ^ s) for i in range(size)])


def tswap(x, s):
    return swap(x, TENSOR, 8, s)


def shape(*dims, dtype=BF):
    return jax.ShapeDtypeStruct(dims, dtype)


def call(kernel, outs, scratch=(), flops=0, limit=32, n_smem=0):
    def run(*args):
        return pl.pallas_call(
            kernel,
            out_shape=outs,
            in_specs=[SMEM] * n_smem + [VMEM] * (len(args) - n_smem),
            out_specs=jax.tree.map(lambda _: VMEM, outs),
            scratch_shapes=list(scratch),
            compiler_params=pltpu.CompilerParams(vmem_limit_bytes=limit * 2**20),
            cost_estimate=pl.CostEstimate(flops=flops, transcendentals=0, bytes_accessed=2**20),
        )(*args)

    return run


def norm_rows(values, gain):
    mean = jnp.mean(values, axis=-1, keepdims=True)
    centred = values - mean
    var = jnp.mean(centred * centred, axis=-1, keepdims=True)
    return centred * lax.rsqrt(var + 1e-05) * gain


def dot(a, b):
    return jnp.dot(a, b, preferred_element_type=F32)


def qkv_kernel(at_ref, tok_ref, gain_ref, w_ref, *refs):
    slabs, bases, (normed, wp) = refs[:4], refs[4:6], refs[6:]
    y, slot = at_ref[0], at_ref[1]
    for r in range(0, TOK, 144):
        rows = tok_ref[r : r + 144, :].astype(F32)
        normed[r : r + 144, :] = norm_rows(rows, gain_ref[...]).astype(BF)
    normed[TOK:PAD, :] = jnp.zeros((PAD - TOK, D), BF)
    for s in range(4):
        for p in range(3):
            src = pl.multiple_of(p * 192 + (y ^ s) * HD, 16)
            wp[s * 144 + p * HD : s * 144 + (p + 1) * HD, :] = w_ref[pl.ds(src, HD), :]
    for j in range(0, PAD, 256):
        res = lax.dot_general(
            wp[...], normed[j : j + 256, :], (((1,), (1,)), ((), ())), preferred_element_type=F32
        )
        for s in range(4):
            for p in range(3):
                part = res[s * 144 + p * HD : s * 144 + (p + 1) * HD]
                if p == 0:
                    part = part * (LOG2E / HD**0.5)
                slabs[s][p, :, j : j + 256] = part.astype(BF)
    for (first, _, rows), base in zip(CHUNKS, bases):
        start = first + slot * rows
        short = start + rows > TOK

        @pl.when(jnp.logical_not(short))
        def _(start=start, rows=rows, base=base):
            base[...] = tok_ref[pl.ds(pl.multiple_of(start, 16), rows), :]

        @pl.when(short)
        def _(first=first, rows=rows, base=base):
            kept = max(0, TOK - (first + 7 * rows))
            base[...] = jnp.zeros((rows, D), BF)
            if kept < rows:
                base[0:kept, :] = tok_ref[TOK - kept : TOK, :]


def attend_kernel(at_ref, *refs, lo, cols, own, n_kv, first, last):
    refs = list(refs)
    slabs = [refs.pop(0) for _ in range(4)]
    kvs = [refs.pop(0) for _ in range(n_kv)]
    carry = None if first else [refs.pop(0) for _ in range(2)]
    outs = [refs.pop(0) for _ in range(1 if last else 2)]
    keys, vals, qs, kmax = refs
    blocks = 4 if own else 4 * n_kv
    off = lo if carry is not None and carry[0].shape[-1] == ALL else 0

    most = jnp.zeros((1, TOK), F32)
    for b in range(blocks):
        pair = slabs[b].at[1:3] if own else kvs[b // 4].at[b % 4]
        kt = pair[0, :, :TOK].astype(F32)
        most = jnp.maximum(most, jnp.sum(kt * kt, axis=0, keepdims=True))
        keys[b] = kt.T.astype(BF)
        vals[b, :HD, :] = pair[1, :, :TOK]
        vals[b, HD:, :] = jnp.ones((16, TOK), BF)
    kmax[0] = jnp.max(most)
    for start, width, _ in CHUNKS:
        for s in range(4):
            at = 4 * start + s * width - lo
            if 0 <= at < cols:
                qs[:, at : at + width] = slabs[s][0, :, start : start + width]

    def finish(i, j, acc, m):
        if not last:
            outs[0][:, pl.ds(j, QW)] = acc
            outs[1][:, pl.ds(j, QW)] = m
            return
        done = (acc[:HD] / acc[HD : HD + 1]).astype(BF)
        half = outs[0].shape[-1]
        for p in range(QW // half):
            source, side = i * (QW // half // 2) + p // 2, p % 2
            to = (at_ref[0] ^ source) * 2 + (at_ref[1] ^ side)
            outs[0][to] = done[:, p * half : (p + 1) * half]

    def tile(i, _):
        j = pl.multiple_of(i * QW, QW)
        qt = qs[:, pl.ds(j, QW)]
        qf = qt.astype(F32)
        safe = jnp.max(jnp.sum(qf * qf, axis=0, keepdims=True)) * kmax[0] <= SAFE
        if first:
            m0, acc0 = jnp.full((1, QW), -1e30, F32), jnp.zeros((64, QW), F32)
        else:
            acc0, m0 = (c[:, pl.ds(pl.multiple_of(off + j, QW), QW)] for c in carry)
            safe = jnp.logical_and(safe, jnp.max(jnp.abs(m0)) == 0.0)

        @pl.when(safe)
        def _():
            acc = acc0
            for b in range(blocks):
                acc = acc + dot(vals[b], jnp.exp2(dot(keys[b], qt)).astype(BF))
            finish(i, j, acc, jnp.zeros((1, QW), F32))

        @pl.when(jnp.logical_not(safe))
        def _():
            def block(b, st):
                m, acc = st
                scores = dot(keys[b], qt)
                fresh = jnp.maximum(m, jnp.max(scores, axis=0, keepdims=True))
                acc = acc * jnp.exp2(m - fresh)
                return fresh, acc + dot(vals[b], jnp.exp2(scores - fresh).astype(BF))

            m, acc = lax.fori_loop(0, blocks, block, (m0, acc0))
            finish(i, j, acc, m)

        return 0

    lax.fori_loop(0, cols // QW, tile, 0)


def attend(at, slabs, kvs, carry, lo, cols, last):
    first, own = carry is None, not kvs
    blocks = 4 * max(1, len(kvs))
    if last:
        outs = shape(8, HD, cols // 8)
    else:
        outs = (shape(64, cols, dtype=F32), shape(1, cols, dtype=F32))
    scratch = [
        pltpu.VMEM((blocks, TOK, HD), BF),
        pltpu.VMEM((blocks, 64, TOK), BF),
        pltpu.VMEM((HD, cols), BF),
        pltpu.SMEM((1,), F32),
    ]
    kernel = functools.partial(
        attend_kernel, lo=lo, cols=cols, own=own, n_kv=len(kvs), first=first, last=last
    )
    flops = cols * blocks * TOK * 8 * HD
    return call(kernel, outs, scratch, flops, 14, n_smem=1)(at, *slabs, *kvs, *(carry or ()))


def mix_kernel(at_ref, got_ref, w_ref, wo_ref, *refs, rows):
    outs, (heads, tall, lhs) = refs[:4], refs[4:]
    xl, g = at_ref[2], at_ref[3]
    for i in range(2):
        for y in range(4):
            heads[y * HD : (y + 1) * HD, :] = got_ref[y * 2 + (xl ^ i)]
        tall[...] = heads[...].astype(F32).T.astype(BF)
        for s in range(4):
            src = pl.multiple_of((g ^ s) * rows, 16)
            lhs[i, s * rows : (s + 1) * rows, :] = tall[pl.ds(src, rows), :]
    for j in range(0, D, 512):
        term = dot(lhs[0], w_ref[:, j : j + 512]) + dot(lhs[1], wo_ref[:, j : j + 512])
        term = term.astype(BF)
        for s in range(4):
            outs[s][:, j : j + 512] = term[s * rows : (s + 1) * rows]


def norm_kernel(base_ref, t0, t1, t2, t3, gain_ref, mixed_ref, post_ref):
    mixed = base_ref[...].astype(F32)
    for t in (t0, t1, t2, t3):
        mixed = mixed + t[...].astype(F32)
    mixed_ref[...] = mixed
    post_ref[...] = norm_rows(mixed, gain_ref[...]).astype(BF)


def ffn_kernel(p0, p1, p2, p3, up, down, ea, eb, *refs, rows):
    outs, (posts, acc) = refs[:4], refs[4:]
    for s, p in enumerate((p0, p1, p2, p3)):
        posts[s * rows : (s + 1) * rows, :] = p[...]
    n = 384

    def hidden(u):
        return jax.nn.gelu(dot(posts[...], u), approximate=True).astype(BF)

    acc[...] = dot(hidden(up[:, :n]), down[:n, :])
    acc[...] += dot(hidden(up[:, n:]), down[n:, :])
    ha, hb = hidden(ea[:D, :]), hidden(eb[:D, :])
    for j in range(4):
        at = D + j * n
        add = dot(ha, ea[at : at + n, :]) + dot(hb, eb[at : at + n, :])
        acc[:, j * n : (j + 1) * n] += add
    for s in range(4):
        outs[s][...] = acc[s * rows : (s + 1) * rows, :].astype(BF)


def sum_kernel(mixed_ref, t0, t1, t2, t3, out_ref):
    total = mixed_ref[...]
    for t in (t0, t1, t2, t3):
        total = total + t[...].astype(F32)
    total = total.astype(BF)
    for i in range(8):
        out_ref[i] = total


def slot_of(t):
    zl, x = t >> 2, t & 3
    return ((x & 1) ^ (x >> 1)) * 4 + zl * 2 + (x >> 1)


def place_kernel(*refs):
    o_ref = refs[2]
    for (first, _, rows), ref in zip(CHUNKS, refs):
        for t in range(8):
            start = first + slot_of(t) * rows
            kept = min(rows, TOK - start)
            o_ref[start : start + kept, :] = ref[t, :kept, :]


def per_device(tokens, norm_gain, w_qkv, w_out, post_gain, w_up, w_down):
    y, core = lax.axis_index("y"), lax.axis_index("core")
    xh, xl = lax.axis_index("xh"), lax.axis_index("xl")
    slot = slot_of(lax.axis_index(TENSOR))
    half = w_up.shape[1] // 2
    at = jnp.stack([y, xh, xl, slot % 4])

    w = jnp.transpose(w_qkv, (1, 2, 0)).reshape(-1, D)
    outs = (shape(3, HD, PAD),) * 4 + tuple(shape(c[2], D) for c in CHUNKS)
    scratch = [pltpu.VMEM((PAD, D), BF), pltpu.VMEM((576, D), BF)]
    *slabs, base0, base1 = call(
        qkv_kernel, outs, scratch, 2 * 576 * D * PAD, 20, n_smem=1
    )(jnp.stack([y, slot]), tokens, norm_gain.reshape(1, D), w)
    slabs = slabs[:1] + [swap(slabs[s], "y", 4, s) for s in range(1, 4)]
    kv = jnp.stack([s[1:] for s in slabs])
    kv_c = swap(kv, "core", 2, 1)
    kv_z = swap(kv, "zh", 2, 1)

    out_a = tswap(w_out, PAIR)
    up_half = lax.dynamic_slice_in_dim(w_up, core * half, half, 1)
    down_half = lax.dynamic_slice_in_dim(w_down, core * half, half, 0)
    down_half = down_half.reshape(half, 4, half).transpose(1, 0, 2).reshape(D, half)
    extra_a = tswap(jnp.concatenate([up_half, down_half], 0), PAIR)

    part = attend(at, slabs, (), None, 0, ALL, False)
    part = attend(at, slabs, (kv_c,), part, 0, ALL, False)
    kv_zc = swap(kv_z, "core", 2, 1)
    heads = [attend(at, slabs, (kv_z, kv_zc), part, 0, 1024, True)]
    part = attend(at, slabs, (kv_z,), part, 1024, 2048, False)
    heads.append(attend(at, slabs, (kv_zc,), part, 1024, 2048, True))
    extra_b = swap(extra_a, "core", 2, 1)

    slabs = []
    for c, (_, cols, rows) in enumerate(CHUNKS):
        got = lax.all_to_all(heads[c], ("y", "xl"), 0, 0)
        four = (shape(rows, D),) * 4
        n = 4 * rows
        scratch = [pltpu.VMEM((192, n), BF), pltpu.VMEM((n, 192), BF), pltpu.VMEM((2, n, 192), BF)]
        kernel = functools.partial(mix_kernel, rows=rows)
        terms = call(kernel, four, scratch, 2 * n * 384 * D, 8, n_smem=1)(at, got, w_out, out_a)
        terms = [terms[0]] + [tswap(terms[i + 1], m) for i, m in enumerate(GROUP)]
        outs = (shape(rows, D, dtype=F32), shape(rows, D))
        mixed, post = call(norm_kernel, outs, limit=6)(
            (base0, base1)[c], *terms, post_gain.reshape(1, D)
        )
        posts = [post] + [tswap(post, m) for m in GROUP]
        scratch = [pltpu.VMEM((n, D), BF), pltpu.VMEM((n, D), F32)]
        kernel = functools.partial(ffn_kernel, rows=rows)
        downs = call(kernel, four, scratch, 8 * n * 768 * D, 20)(
            *posts, w_up, w_down, extra_a, extra_b
        )
        downs = [downs[0]] + [tswap(downs[i + 1], m) for i, m in enumerate(GROUP)]
        final = call(sum_kernel, shape(8, rows, D), limit=8)(mixed, *downs)
        slabs.append(lax.all_to_all(final, TENSOR, 0, 0))
    return call(place_kernel, shape(TOK, D), limit=12)(*slabs)


def solution(mesh):
    seq, ten = ("zh", "y", "core"), TENSOR
    fine = Mesh(mesh.devices.reshape(2, 4, 2, 2, 2, 2), seq + ten)
    placed = (P(seq, None), P(), P(None, None, ten), P(ten, None), P(), P(None, ten), P(ten, None))

    return jax.shard_map(
        per_device, mesh=fine, in_specs=placed, out_specs=P(seq, None), check_vma=False
    )
```

```python
import functools

import jax
import jax.numpy as jnp
from jax import lax
from jax.experimental import pallas as pl
from jax.experimental.pallas import tpu as pltpu
from jax.sharding import Mesh
from jax.sharding import PartitionSpec as P


HD = 48
D = 1536
TOK = 720
PAD = 768
QW = 512
ALL = 4 * PAD
CHUNKS = ((0, 256, 32), (256, 512, 64))
LOG2E = 1.4426950408889634
SAFE = 90.0 * 90.0
BF = jnp.bfloat16
F32 = jnp.float32
VMEM = pl.BlockSpec(memory_space=pltpu.VMEM)
SMEM = pl.BlockSpec(memory_space=pltpu.SMEM)
PAIR = 1
TENSOR = ("zl", "xh", "xl")
Y, CORE, SIDE, SLOT, GROUP_AT, T = range(6)
GROUP = (3, 4, 7)


def swap(x, axis, size, s):
    return lax.ppermute(x, axis, [(i, i ^ s) for i in range(size)])


def tswap(x, s):
    return swap(x, TENSOR, 8, s)


def shape(*dims, dtype=BF):
    return jax.ShapeDtypeStruct(dims, dtype)


def call(kernel, outs, scratch=(), flops=0, limit=32, n_smem=0):
    def run(*args):
        return pl.pallas_call(
            kernel,
            out_shape=outs,
            in_specs=[SMEM] * n_smem + [VMEM] * (len(args) - n_smem),
            out_specs=jax.tree.map(lambda _: VMEM, outs),
            scratch_shapes=list(scratch),
            compiler_params=pltpu.CompilerParams(vmem_limit_bytes=limit * 2**20),
            cost_estimate=pl.CostEstimate(flops=flops, transcendentals=0, bytes_accessed=2**20),
        )(*args)

    return run


def norm_rows(values, gain):
    mean = jnp.mean(values, axis=-1, keepdims=True)
    centred = values - mean
    var = jnp.mean(centred * centred, axis=-1, keepdims=True)
    return centred * lax.rsqrt(var + 1e-05) * gain


def dot(a, b):
    return jnp.dot(a, b, preferred_element_type=F32)


def qkv_kernel(at_ref, tok_ref, gain_ref, w_ref, *refs):
    slabs, bases, (normed, wp) = refs[:4], refs[4:6], refs[6:]
    y, slot = at_ref[Y], at_ref[SLOT]
    for r in range(0, TOK, 144):
        rows = tok_ref[r : r + 144, :].astype(F32)
        normed[r : r + 144, :] = norm_rows(rows, gain_ref[...].reshape(1, D)).astype(BF)
    normed[TOK:PAD, :] = jnp.zeros((PAD - TOK, D), BF)
    for s in range(4):
        for p in range(3):
            src = pl.multiple_of(p * 192 + (y ^ s) * HD, 16)
            wp[s * 144 + p * HD : s * 144 + (p + 1) * HD, :] = w_ref[pl.ds(src, HD), :]
    for j in range(0, PAD, 256):
        res = lax.dot_general(
            wp[...], normed[j : j + 256, :], (((1,), (1,)), ((), ())), preferred_element_type=F32
        )
        for s in range(4):
            for p in range(3):
                part = res[s * 144 + p * HD : s * 144 + (p + 1) * HD]
                if p == 0:
                    part = part * (LOG2E / HD**0.5)
                slabs[s][p, :, j : j + 256] = part.astype(BF)
    for (first, _, rows), base in zip(CHUNKS, bases):
        start = first + slot * rows
        short = start + rows > TOK

        @pl.when(jnp.logical_not(short))
        def _(start=start, rows=rows, base=base):
            base[...] = tok_ref[pl.ds(pl.multiple_of(start, 16), rows), :]

        @pl.when(short)
        def _(first=first, rows=rows, base=base):
            kept = max(0, TOK - (first + 7 * rows))
            base[...] = jnp.zeros((rows, D), BF)
            if kept < rows:
                base[0:kept, :] = tok_ref[TOK - kept : TOK, :]


def attend_kernel(at_ref, *refs, lo, cols, own, n_kv, first, last):
    refs = list(refs)
    slabs = [refs.pop(0) for _ in range(4)]
    kvs = [refs.pop(0) for _ in range(n_kv)]
    carry = None if first else [refs.pop(0) for _ in range(2)]
    outs = [refs.pop(0) for _ in range(4 if last else 2)]
    keys, vals, qs, kmax = refs[:4]
    final = refs[4] if last else None
    blocks = 4 if own else 4 * n_kv
    off = lo if carry is not None and carry[0].shape[-1] == ALL else 0

    most = jnp.zeros((1, TOK), F32)
    for b in range(blocks):
        pair = slabs[b].at[1:3] if own else kvs[b // 4].at[b % 4]
        kt = pair[0, :, :TOK].astype(F32)
        most = jnp.maximum(most, jnp.sum(kt * kt, axis=0, keepdims=True))
        keys[b] = kt.T.astype(BF)
        vals[b, :HD, :] = pair[1, :, :TOK]
        vals[b, HD:, :] = jnp.ones((16, TOK), BF)
    kmax[0] = jnp.max(most)
    for start, width, _ in CHUNKS:
        for s in range(4):
            at = 4 * start + s * width - lo
            if 0 <= at < cols:
                qs[:, at : at + width] = slabs[s][0, :, start : start + width]

    def finish(i, j, acc, m):
        if not last:
            outs[0][:, pl.ds(j, QW)] = acc
            outs[1][:, pl.ds(j, QW)] = m
            return
        done = (acc[:HD] / acc[HD : HD + 1]).astype(BF)
        half = final.shape[-1]
        for p in range(QW // half):
            source, side = i * (QW // half // 2) + p // 2, p % 2
            final[source, at_ref[SIDE] ^ side] = done[:, p * half : (p + 1) * half]

    def tile(i, _):
        j = pl.multiple_of(i * QW, QW)
        qt = qs[:, pl.ds(j, QW)]
        qf = qt.astype(F32)
        safe = jnp.max(jnp.sum(qf * qf, axis=0, keepdims=True)) * kmax[0] <= SAFE
        if first:
            m0, acc0 = jnp.full((1, QW), -1e30, F32), jnp.zeros((64, QW), F32)
        else:
            acc0, m0 = (c[:, pl.ds(pl.multiple_of(off + j, QW), QW)] for c in carry)
            safe = jnp.logical_and(safe, jnp.max(jnp.abs(m0)) == 0.0)

        @pl.when(safe)
        def _():
            acc = acc0
            for b in range(blocks):
                acc = acc + dot(vals[b], jnp.exp2(dot(keys[b], qt)).astype(BF))
            finish(i, j, acc, jnp.zeros((1, QW), F32))

        @pl.when(jnp.logical_not(safe))
        def _():
            def block(b, st):
                m, acc = st
                scores = dot(keys[b], qt)
                fresh = jnp.maximum(m, jnp.max(scores, axis=0, keepdims=True))
                acc = acc * jnp.exp2(m - fresh)
                return fresh, acc + dot(vals[b], jnp.exp2(scores - fresh).astype(BF))

            m, acc = lax.fori_loop(0, blocks, block, (m0, acc0))
            finish(i, j, acc, m)

        return 0

    lax.fori_loop(0, cols // QW, tile, 0)
    if last:
        for s in range(4):
            outs[s][...] = final[s]


def attend(at, slabs, kvs, carry, lo, cols, last):
    first, own = carry is None, not kvs
    blocks = 4 * max(1, len(kvs))
    if last:
        outs = (shape(2, HD, cols // 8),) * 4
    else:
        outs = (shape(64, cols, dtype=F32), shape(1, cols, dtype=F32))
    scratch = [
        pltpu.VMEM((blocks, TOK, HD), BF),
        pltpu.VMEM((blocks, 64, TOK), BF),
        pltpu.VMEM((HD, cols), BF),
        pltpu.SMEM((1,), F32),
    ]
    if last:
        scratch.append(pltpu.VMEM((4, 2, HD, cols // 8), BF))
    kernel = functools.partial(
        attend_kernel, lo=lo, cols=cols, own=own, n_kv=len(kvs), first=first, last=last
    )
    flops = cols * blocks * TOK * 8 * HD
    return call(kernel, outs, scratch, flops, 14, n_smem=1)(at, *slabs, *kvs, *(carry or ()))


def mix_kernel(at_ref, b0, b1, b2, b3, other_ref, w_ref, wo_ref, *refs, rows):
    outs, (heads, tall, lhs) = refs[:4], refs[4:]
    y, g = at_ref[Y], at_ref[GROUP_AT]
    for i in range(2):
        for s, back in enumerate((b0, b1, b2, b3)):
            to = pl.ds(pl.multiple_of((y ^ s) * HD, 16), HD)
            heads[to, :] = other_ref[s] if i else back[0]
        tall[...] = heads[...].astype(F32).T.astype(BF)
        for s in range(4):
            src = pl.multiple_of((g ^ s) * rows, 16)
            lhs[i, s * rows : (s + 1) * rows, :] = tall[pl.ds(src, rows), :]
    for j in range(0, D, 512):
        term = dot(lhs[0], w_ref[:, j : j + 512]) + dot(lhs[1], wo_ref[:, j : j + 512])
        term = term.astype(BF)
        for s in range(4):
            outs[s][:, j : j + 512] = term[s * rows : (s + 1) * rows]


def norm_kernel(base_ref, t0, t1, t2, t3, gain_ref, mixed_ref, post_ref):
    mixed = base_ref[...].astype(F32)
    for t in (t0, t1, t2, t3):
        mixed = mixed + t[...].astype(F32)
    mixed_ref[...] = mixed
    post_ref[...] = norm_rows(mixed, gain_ref[...].reshape(1, D)).astype(BF)


def ffn_kernel(p0, p1, p2, p3, up, down, ea, eb, *refs, rows):
    outs, (posts, acc) = refs[:4], refs[4:]
    for s, p in enumerate((p0, p1, p2, p3)):
        posts[s * rows : (s + 1) * rows, :] = p[...]
    n = 384

    def hidden(u):
        return jax.nn.gelu(dot(posts[...], u), approximate=True).astype(BF)

    acc[...] = dot(hidden(up[:, :n]), down[:n, :])
    acc[...] += dot(hidden(up[:, n:]), down[n:, :])
    ha, hb = hidden(ea[:D, :]), hidden(eb[:D, :])
    for j in range(4):
        at = D + j * n
        add = dot(ha, ea[at : at + n, :]) + dot(hb, eb[at : at + n, :])
        acc[:, j * n : (j + 1) * n] += add
    for s in range(4):
        outs[s][...] = acc[s * rows : (s + 1) * rows, :].astype(BF)


def sum_kernel(mixed_ref, t0, t1, t2, t3, out_ref):
    total = mixed_ref[...]
    for t in (t0, t1, t2, t3):
        total = total + t[...].astype(F32)
    out_ref[...] = total.astype(BF)


def slot_of(t):
    zl, x = t >> 2, t & 3
    return ((x & 1) ^ (x >> 1)) * 4 + zl * 2 + (x >> 1)


def pack_kernel(at_ref, up_ref, down_ref, out_ref):
    n = out_ref.shape[1]
    at = pl.multiple_of(at_ref[CORE] * n, 128)
    out_ref[:D, :] = up_ref[:, pl.ds(at, n)]
    for j in range(4):
        out_ref[D + j * n : D + (j + 1) * n, :] = down_ref[pl.ds(at, n), j * n : (j + 1) * n]


def place_kernel(at_ref, *refs):
    o_ref = refs[-1]
    first = [refs[i // 2].at[i % 2] for i in (0, 2, 4, 6, 1, 3, 5, 7)]
    pieces = (first, refs[4:12])
    for (begin, _, rows), slabs in zip(CHUNKS, pieces):
        for s, slab in enumerate(slabs):
            start = begin + slot_of(at_ref[T] ^ s) * rows
            kept = TOK - (begin + 7 * rows)
            if kept >= rows:
                o_ref[pl.ds(pl.multiple_of(start, 16), rows), :] = slab[...]
                continue
            short = start + rows > TOK

            @pl.when(jnp.logical_not(short))
            def _(slab=slab, start=start, rows=rows):
                o_ref[pl.ds(pl.multiple_of(start, 16), rows), :] = slab[...]

            @pl.when(short)
            def _(slab=slab, kept=kept):
                o_ref[TOK - kept : TOK, :] = slab[:kept, :]


def per_device(tokens, norm_gain, w_qkv, w_out, post_gain, w_up, w_down):
    t = lax.axis_index(TENSOR)
    slot = slot_of(t)
    at = jnp.stack([lax.axis_index("y"), lax.axis_index("core"), slot // 4, slot, slot % 4, t])

    w = jnp.transpose(w_qkv, (1, 2, 0)).reshape(-1, D)
    outs = (shape(3, HD, PAD),) * 4 + tuple(shape(c[2], D) for c in CHUNKS)
    scratch = [pltpu.VMEM((PAD, D), BF), pltpu.VMEM((576, D), BF)]
    *slabs, base0, base1 = call(
        qkv_kernel, outs, scratch, 2 * 576 * D * PAD, 20, n_smem=1
    )(at, tokens, norm_gain, w)
    slabs = slabs[:1] + [swap(slabs[s], "y", 4, s) for s in range(1, 4)]
    kv = jnp.stack([s[1:] for s in slabs])
    kv_c = swap(kv, "core", 2, 1)
    kv_z = swap(kv, "zh", 2, 1)

    out_a = tswap(w_out, PAIR)
    packed = call(pack_kernel, shape(2 * D, w_up.shape[1] // 2), flops=2**28, limit=16, n_smem=1)(
        at, w_up, w_down
    )
    extra_a = tswap(packed, PAIR)

    part = attend(at, slabs, (), None, 0, ALL, False)
    part = attend(at, slabs, (kv_c,), part, 0, ALL, False)
    kv_zc = swap(kv_z, "core", 2, 1)
    heads = [attend(at, slabs, (kv_z, kv_zc), part, 0, 1024, True)]
    part = attend(at, slabs, (kv_z,), part, 1024, 2048, False)
    heads.append(attend(at, slabs, (kv_zc,), part, 1024, 2048, True))
    extra_b = swap(extra_a, "core", 2, 1)

    slabs = []
    for c, (_, cols, rows) in enumerate(CHUNKS):
        back = [heads[c][0]] + [swap(heads[c][s], "y", 4, s) for s in range(1, 4)]
        give = jnp.stack([b[1] for b in back])
        other = tswap(give, PAIR)
        four = (shape(rows, D),) * 4
        n = 4 * rows
        scratch = [pltpu.VMEM((192, n), BF), pltpu.VMEM((n, 192), BF), pltpu.VMEM((2, n, 192), BF)]
        kernel = functools.partial(mix_kernel, rows=rows)
        terms = call(kernel, four, scratch, 2 * n * 384 * D, 8, n_smem=1)(
            at, *back, other, w_out, out_a
        )
        terms = [terms[0]] + [tswap(terms[i + 1], m) for i, m in enumerate(GROUP)]
        outs = (shape(rows, D, dtype=F32), shape(rows, D))
        mixed, post = call(norm_kernel, outs, limit=6)((base0, base1)[c], *terms, post_gain)
        posts = [post] + [tswap(post, m) for m in GROUP]
        scratch = [pltpu.VMEM((n, D), BF), pltpu.VMEM((n, D), F32)]
        kernel = functools.partial(ffn_kernel, rows=rows)
        downs = call(kernel, four, scratch, 8 * n * 768 * D, 20)(
            *posts, w_up, w_down, extra_a, extra_b
        )
        downs = [downs[0]] + [tswap(downs[i + 1], m) for i, m in enumerate(GROUP)]
        final = call(sum_kernel, shape(rows, D), limit=4)(mixed, *downs)
        if c == 0:
            both = jnp.stack([final, tswap(final, 4)])
            slabs = [both] + [tswap(both, s) for s in range(1, 4)]
        else:
            slabs += [final] + [tswap(final, s) for s in range(1, 8)]
    return call(place_kernel, shape(TOK, D), limit=12, n_smem=1)(at, *slabs)


def solution(mesh):
    seq, ten = ("zh", "y", "core"), TENSOR
    fine = Mesh(mesh.devices.reshape(2, 4, 2, 2, 2, 2), seq + ten)
    placed = (P(seq, None), P(), P(None, None, ten), P(ten, None), P(), P(None, ten), P(ten, None))

    return jax.shard_map(
        per_device, mesh=fine, in_specs=placed, out_specs=P(seq, None), check_vma=False
    )
```

```python
import functools

import jax
import jax.numpy as jnp
from jax import lax
from jax.experimental import pallas as pl
from jax.experimental.pallas import tpu as pltpu
from jax.sharding import Mesh
from jax.sharding import PartitionSpec as P


HD = 48
D = 1536
TOK = 720
PAD = 768
QW = 512
ALL = 4 * PAD
CHUNKS = ((0, 256, 32), (256, 512, 64))
LOG2E = 1.4426950408889634
SAFE = 90.0 * 90.0
BF = jnp.bfloat16
F32 = jnp.float32
VMEM = pl.BlockSpec(memory_space=pltpu.VMEM)
SMEM = pl.BlockSpec(memory_space=pltpu.SMEM)
ANY = pl.BlockSpec(memory_space=pltpu.HBM)
PAIR = 1
TENSOR = ("zl", "xh", "xl")
Y, CORE, SIDE, SLOT, GROUP_AT, T = range(6)
GROUP = (3, 4, 7)


def swap(x, axis, size, s):
    return lax.ppermute(x, axis, [(i, i ^ s) for i in range(size)])


def tswap(x, s):
    return swap(x, TENSOR, 8, s)


def shape(*dims, dtype=BF):
    return jax.ShapeDtypeStruct(dims, dtype)


def call(kernel, outs, scratch=(), flops=0, limit=32, n_smem=0, n_any=0):
    def run(*args):
        return pl.pallas_call(
            kernel,
            out_shape=outs,
            in_specs=[SMEM] * n_smem + [ANY] * n_any + [VMEM] * (len(args) - n_smem - n_any),
            out_specs=jax.tree.map(lambda _: VMEM, outs),
            scratch_shapes=list(scratch),
            compiler_params=pltpu.CompilerParams(vmem_limit_bytes=limit * 2**20),
            cost_estimate=pl.CostEstimate(flops=flops, transcendentals=0, bytes_accessed=2**20),
        )(*args)

    return run


def norm_rows(values, gain):
    mean = jnp.mean(values, axis=-1, keepdims=True)
    centred = values - mean
    var = jnp.mean(centred * centred, axis=-1, keepdims=True)
    return centred * lax.rsqrt(var + 1e-05) * gain


def dot(a, b):
    return jnp.dot(a, b, preferred_element_type=F32)


def qkv_kernel(at_ref, tok_hbm, gain_hbm, w_hbm, *refs):
    slabs, bases = refs[:4], refs[4:6]
    normed, wp, tok_ref, gain_ref, w_ref, sems = refs[6:]
    y, slot = at_ref[Y], at_ref[SLOT]
    copies = [pltpu.make_async_copy(gain_hbm, gain_ref, sems.at[0])]
    for i in range(5):
        rows = pl.ds(i * 144, 144)
        copies.append(pltpu.make_async_copy(tok_hbm.at[rows], tok_ref.at[rows], sems.at[1 + i]))
    copies.append(pltpu.make_async_copy(w_hbm, w_ref, sems.at[6]))
    for copy in copies:
        copy.start()
    copies[0].wait()
    for r in range(0, TOK, 144):
        copies[1 + r // 144].wait()
        rows = tok_ref[r : r + 144, :].astype(F32)
        normed[r : r + 144, :] = norm_rows(rows, gain_ref[...].reshape(1, D)).astype(BF)
    normed[TOK:PAD, :] = jnp.zeros((PAD - TOK, D), BF)
    copies[6].wait()
    for s in range(4):
        for p in range(3):
            src = pl.multiple_of(p * 192 + (y ^ s) * HD, 16)
            wp[s * 144 + p * HD : s * 144 + (p + 1) * HD, :] = w_ref[pl.ds(src, HD), :]
    for j in range(0, PAD, 256):
        res = lax.dot_general(
            wp[...], normed[j : j + 256, :], (((1,), (1,)), ((), ())), preferred_element_type=F32
        )
        for s in range(4):
            for p in range(3):
                part = res[s * 144 + p * HD : s * 144 + (p + 1) * HD]
                if p == 0:
                    part = part * (LOG2E / HD**0.5)
                slabs[s][p, :, j : j + 256] = part.astype(BF)
    for (first, _, rows), base in zip(CHUNKS, bases):
        start = first + slot * rows
        short = start + rows > TOK

        @pl.when(jnp.logical_not(short))
        def _(start=start, rows=rows, base=base):
            base[...] = tok_ref[pl.ds(pl.multiple_of(start, 16), rows), :]

        @pl.when(short)
        def _(first=first, rows=rows, base=base):
            kept = max(0, TOK - (first + 7 * rows))
            base[...] = jnp.zeros((rows, D), BF)
            if kept < rows:
                base[0:kept, :] = tok_ref[TOK - kept : TOK, :]


def attend_kernel(at_ref, *refs, lo, cols, sets, first, last):
    refs = list(refs)
    slabs = [refs.pop(0) for _ in range(4)]
    kvs = refs.pop(0) if sets else None
    carry = None if first else [refs.pop(0) for _ in range(2)]
    outs = [refs.pop(0) for _ in range(4 if last else 2)]
    keys, vals, qs, kmax = refs[:4]
    final = refs[4] if last else None
    blocks = 4 * max(1, sets)
    off = lo if carry is not None and carry[0].shape[-1] == ALL else 0

    most = jnp.zeros((1, TOK), F32)
    for b in range(blocks):
        pair = kvs.at[b // 4, b % 4] if sets else slabs[b].at[1:3]
        kt = pair[0, :, :TOK].astype(F32)
        most = jnp.maximum(most, jnp.sum(kt * kt, axis=0, keepdims=True))
        keys[b] = kt.T.astype(BF)
        vals[b, :HD, :] = pair[1, :, :TOK]
        vals[b, HD:, :] = jnp.ones((16, TOK), BF)
    kmax[0] = jnp.max(most)
    for start, width, _ in CHUNKS:
        for s in range(4):
            at = 4 * start + s * width - lo
            if 0 <= at < cols:
                qs[:, at : at + width] = slabs[s][0, :, start : start + width]

    def finish(i, j, acc, m):
        if not last:
            outs[0][:, pl.ds(j, QW)] = acc
            outs[1][:, pl.ds(j, QW)] = m
            return
        done = (acc[:HD] / acc[HD : HD + 1]).astype(BF)
        half = final.shape[-1]
        for p in range(QW // half):
            source, side = i * (QW // half // 2) + p // 2, p % 2
            final[source, at_ref[SIDE] ^ side] = done[:, p * half : (p + 1) * half]

    def tile(i, _):
        j = pl.multiple_of(i * QW, QW)
        qt = qs[:, pl.ds(j, QW)]
        qf = qt.astype(F32)
        safe = jnp.max(jnp.sum(qf * qf, axis=0, keepdims=True)) * kmax[0] <= SAFE
        if first:
            m0, acc0 = jnp.full((1, QW), -1e30, F32), jnp.zeros((64, QW), F32)
        else:
            acc0, m0 = (c[:, pl.ds(pl.multiple_of(off + j, QW), QW)] for c in carry)
            safe = jnp.logical_and(safe, jnp.max(jnp.abs(m0)) == 0.0)

        @pl.when(safe)
        def _():
            acc, scores = acc0, dot(keys[0], qt)
            for b in range(blocks):
                ahead = dot(keys[b + 1], qt) if b + 1 < blocks else None
                acc = acc + dot(vals[b], jnp.exp2(scores).astype(BF))
                scores = ahead
            finish(i, j, acc, jnp.zeros((1, QW), F32))

        @pl.when(jnp.logical_not(safe))
        def _():
            def block(b, st):
                m, acc = st
                scores = dot(keys[b], qt)
                fresh = jnp.maximum(m, jnp.max(scores, axis=0, keepdims=True))
                acc = acc * jnp.exp2(m - fresh)
                return fresh, acc + dot(vals[b], jnp.exp2(scores - fresh).astype(BF))

            m, acc = lax.fori_loop(0, blocks, block, (m0, acc0))
            finish(i, j, acc, m)

        return 0

    lax.fori_loop(0, cols // QW, tile, 0)
    if last:
        for s in range(4):
            outs[s][...] = final[s]


def attend(at, slabs, kvs, carry, lo, cols, last):
    first, sets = carry is None, 0 if kvs is None else kvs.shape[0]
    blocks = 4 * max(1, sets)
    if last:
        outs = (shape(2, HD, cols // 8),) * 4
    else:
        outs = (shape(64, cols, dtype=F32), shape(1, cols, dtype=F32))
    scratch = [
        pltpu.VMEM((blocks, TOK, HD), BF),
        pltpu.VMEM((blocks, 64, TOK), BF),
        pltpu.VMEM((HD, cols), BF),
        pltpu.SMEM((1,), F32),
    ]
    if last:
        scratch.append(pltpu.VMEM((4, 2, HD, cols // 8), BF))
    kernel = functools.partial(
        attend_kernel, lo=lo, cols=cols, sets=sets, first=first, last=last
    )
    flops = cols * blocks * TOK * 8 * HD
    return call(kernel, outs, scratch, flops, 14, n_smem=1)(
        at, *slabs, *(() if kvs is None else (kvs,)), *(carry or ())
    )


def mix_kernel(at_ref, b0, b1, b2, b3, other_ref, w_ref, wo_ref, *refs, rows):
    outs, (heads, tall, lhs) = refs[:4], refs[4:]
    y, g = at_ref[Y], at_ref[GROUP_AT]
    for i in range(2):
        for s, back in enumerate((b0, b1, b2, b3)):
            to = pl.ds(pl.multiple_of((y ^ s) * HD, 16), HD)
            heads[to, :] = other_ref[s] if i else back[0]
        tall[...] = heads[...].astype(F32).T.astype(BF)
        for s in range(4):
            src = pl.multiple_of((g ^ s) * rows, 16)
            lhs[i, s * rows : (s + 1) * rows, :] = tall[pl.ds(src, rows), :]
    for j in range(0, D, 512):
        term = dot(lhs[0], w_ref[:, j : j + 512]) + dot(lhs[1], wo_ref[:, j : j + 512])
        term = term.astype(BF)
        for s in range(4):
            outs[s][:, j : j + 512] = term[s * rows : (s + 1) * rows]


def norm_kernel(base_ref, t0, t1, t2, t3, gain_ref, mixed_ref, post_ref):
    mixed = base_ref[...].astype(F32)
    for t in (t0, t1, t2, t3):
        mixed = mixed + t[...].astype(F32)
    mixed_ref[...] = mixed
    post_ref[...] = norm_rows(mixed, gain_ref[...].reshape(1, D)).astype(BF)


def ffn_kernel(p0, p1, p2, p3, up, down, ea, eb, *refs, rows):
    outs, (posts, acc) = refs[:4], refs[4:]
    for s, p in enumerate((p0, p1, p2, p3)):
        posts[s * rows : (s + 1) * rows, :] = p[...]
    n = 384

    def hidden(u):
        return jax.nn.gelu(dot(posts[...], u), approximate=True).astype(BF)

    acc[...] = dot(hidden(up[:, :n]), down[:n, :])
    acc[...] += dot(hidden(up[:, n:]), down[n:, :])
    ha, hb = hidden(ea[:D, :]), hidden(eb[:D, :])
    for j in range(4):
        at = D + j * n
        add = dot(ha, ea[at : at + n, :]) + dot(hb, eb[at : at + n, :])
        acc[:, j * n : (j + 1) * n] += add
    for s in range(4):
        outs[s][...] = acc[s * rows : (s + 1) * rows, :].astype(BF)


def sum_kernel(mixed_ref, t0, t1, t2, t3, out_ref):
    total = mixed_ref[...]
    for t in (t0, t1, t2, t3):
        total = total + t[...].astype(F32)
    out_ref[...] = total.astype(BF)


def slot_of(t):
    zl, x = t >> 2, t & 3
    return ((x & 1) ^ (x >> 1)) * 4 + zl * 2 + (x >> 1)


def pack_kernel(at_ref, up_ref, down_ref, out_ref):
    n = out_ref.shape[1]
    at = pl.multiple_of(at_ref[CORE] * n, 128)
    out_ref[:D, :] = up_ref[:, pl.ds(at, n)]
    for j in range(4):
        out_ref[D + j * n : D + (j + 1) * n, :] = down_ref[pl.ds(at, n), j * n : (j + 1) * n]


def place_kernel(at_ref, *refs):
    o_ref = refs[-1]
    own, by1, by3, by2, by6 = refs[:5]
    first = [own.at[0], by1.at[0], by2, by3.at[0], own.at[1], by1.at[1], by6, by3.at[1]]
    pieces = (first, refs[5:13])
    for (begin, _, rows), slabs in zip(CHUNKS, pieces):
        for s, slab in enumerate(slabs):
            start = begin + slot_of(at_ref[T] ^ s) * rows
            kept = TOK - (begin + 7 * rows)
            if kept >= rows:
                o_ref[pl.ds(pl.multiple_of(start, 16), rows), :] = slab[...]
                continue
            short = start + rows > TOK

            @pl.when(jnp.logical_not(short))
            def _(slab=slab, start=start, rows=rows):
                o_ref[pl.ds(pl.multiple_of(start, 16), rows), :] = slab[...]

            @pl.when(short)
            def _(slab=slab, kept=kept):
                o_ref[TOK - kept : TOK, :] = slab[:kept, :]


def per_device(tokens, norm_gain, w_qkv, w_out, post_gain, w_up, w_down):
    t = lax.axis_index(TENSOR)
    slot = slot_of(t)
    at = jnp.stack([lax.axis_index("y"), lax.axis_index("core"), slot // 4, slot, slot % 4, t])

    w = jnp.transpose(w_qkv, (1, 2, 0)).reshape(-1, D)
    outs = (shape(3, HD, PAD),) * 4 + tuple(shape(c[2], D) for c in CHUNKS)
    scratch = [
        pltpu.VMEM((PAD, D), BF),
        pltpu.VMEM((576, D), BF),
        pltpu.VMEM((TOK, D), BF),
        pltpu.VMEM((D,), F32),
        pltpu.VMEM((576, D), BF),
        pltpu.SemaphoreType.DMA((7,)),
    ]
    *slabs, base0, base1 = call(
        qkv_kernel, outs, scratch, 2 * 576 * D * PAD, 52, n_smem=1, n_any=3
    )(at, tokens, norm_gain, w)
    far = swap(slabs[2], "y", 4, 2)
    slabs = [slabs[0], swap(slabs[1], "y", 4, 1), far, swap(slabs[3], "y", 4, 3)]
    kv = jnp.stack([s[1:] for s in slabs])
    kv_z = swap(kv, "zh", 2, 1)

    out_a = tswap(w_out, PAIR)
    packed = call(pack_kernel, shape(2 * D, w_up.shape[1] // 2), flops=2**28, limit=16, n_smem=1)(
        at, w_up, w_down
    )
    extra_a = tswap(packed, PAIR)

    part = attend(at, slabs, None, None, 0, ALL, False)
    kv_core = swap(jnp.stack([kv, kv_z]), "core", 2, 1)
    part = attend(at, slabs, kv_z[None], part, 0, ALL, False)
    heads = [
        attend(at, slabs, kv_core, part, 0, 1024, True),
        attend(at, slabs, kv_core, part, 1024, 2048, True),
    ]
    extra_b = swap(extra_a, "core", 2, 1)

    slabs = []
    for c, (_, cols, rows) in enumerate(CHUNKS):
        back = [heads[c][0]] + [swap(heads[c][s], "y", 4, s) for s in range(1, 4)]
        give = jnp.stack([b[1] for b in back])
        other = tswap(give, PAIR)
        four = (shape(rows, D),) * 4
        n = 4 * rows
        scratch = [pltpu.VMEM((192, n), BF), pltpu.VMEM((n, 192), BF), pltpu.VMEM((2, n, 192), BF)]
        kernel = functools.partial(mix_kernel, rows=rows)
        terms = call(kernel, four, scratch, 2 * n * 384 * D, 8, n_smem=1)(
            at, *back, other, w_out, out_a
        )
        terms = [terms[0]] + [tswap(terms[i + 1], m) for i, m in enumerate(GROUP)]
        outs = (shape(rows, D, dtype=F32), shape(rows, D))
        mixed, post = call(norm_kernel, outs, limit=6)((base0, base1)[c], *terms, post_gain)
        posts = [post] + [tswap(post, m) for m in GROUP]
        scratch = [pltpu.VMEM((n, D), BF), pltpu.VMEM((n, D), F32)]
        kernel = functools.partial(ffn_kernel, rows=rows)
        downs = call(kernel, four, scratch, 8 * n * 768 * D, 20)(
            *posts, w_up, w_down, extra_a, extra_b
        )
        downs = [downs[0]] + [tswap(downs[i + 1], m) for i, m in enumerate(GROUP)]
        final = call(sum_kernel, shape(rows, D), limit=4)(mixed, *downs)
        if c == 0:
            both = jnp.stack([final, tswap(final, 4)])
            by1, by3 = tswap(both, 1), tswap(both, 3)
            slabs = [both, by1, by3, tswap(by3[0], 1), tswap(by1[1], 3)]
        else:
            by3, by5 = tswap(final, 3), tswap(final, 5)
            by1, by7, by4 = (tswap(final, s) for s in (1, 7, 4))
            slabs += [final, by1, tswap(by3, 1), by3, by4, by5, tswap(by5, 3), by7]
    return call(place_kernel, shape(TOK, D), limit=12, n_smem=1)(at, *slabs)


def solution(mesh):
    seq, ten = ("zh", "y", "core"), TENSOR
    fine = Mesh(mesh.devices.reshape(2, 4, 2, 2, 2, 2), seq + ten)
    placed = (P(seq, None), P(), P(None, None, ten), P(ten, None), P(), P(None, ten), P(ten, None))

    return jax.shard_map(
        per_device, mesh=fine, in_specs=placed, out_specs=P(seq, None), check_vma=False
    )
```

```python
import functools

import jax
import jax.numpy as jnp
from jax import lax
from jax.experimental import pallas as pl
from jax.experimental.pallas import tpu as pltpu
from jax.sharding import Mesh
from jax.sharding import PartitionSpec as P


HD = 48
D = 1536
TOK = 720
PAD = 768
QW = 512
ALL = 4 * PAD
CHUNKS = ((0, 256, 32), (256, 512, 64))
LOG2E = 1.4426950408889634
SAFE = 90.0 * 90.0
BF = jnp.bfloat16
F32 = jnp.float32
VMEM = pl.BlockSpec(memory_space=pltpu.VMEM)
SMEM = pl.BlockSpec(memory_space=pltpu.SMEM)
ANY = pl.BlockSpec(memory_space=pltpu.HBM)
PAIR = 1
TENSOR = ("zl", "xh", "xl")
Y, CORE, SIDE, SLOT, GROUP_AT, T = range(6)
GROUP = (3, 4, 7)


def swap(x, axis, size, s):
    return lax.ppermute(x, axis, [(i, i ^ s) for i in range(size)])


def tswap(x, s):
    return swap(x, TENSOR, 8, s)


def shape(*dims, dtype=BF):
    return jax.ShapeDtypeStruct(dims, dtype)


def call(kernel, outs, scratch=(), flops=0, limit=32, n_smem=0, n_any=0, out=VMEM):
    def run(*args):
        return pl.pallas_call(
            kernel,
            out_shape=outs,
            in_specs=[SMEM] * n_smem + [ANY] * n_any + [VMEM] * (len(args) - n_smem - n_any),
            out_specs=jax.tree.map(lambda _: out, outs),
            scratch_shapes=list(scratch),
            compiler_params=pltpu.CompilerParams(vmem_limit_bytes=limit * 2**20),
            cost_estimate=pl.CostEstimate(flops=flops, transcendentals=0, bytes_accessed=2**20),
        )(*args)

    return run


def norm_rows(values, gain):
    mean = jnp.mean(values, axis=-1, keepdims=True)
    centred = values - mean
    var = jnp.mean(centred * centred, axis=-1, keepdims=True)
    return centred * lax.rsqrt(var + 1e-05) * gain


def dot(a, b):
    return jnp.dot(a, b, preferred_element_type=F32)


def qkv_kernel(at_ref, tok_hbm, gain_hbm, w_hbm, *refs):
    slabs, bases = refs[:4], refs[4:6]
    normed, wp, tok_ref, gain_ref, w_ref, sems = refs[6:]
    y, slot = at_ref[Y], at_ref[SLOT]
    copies = [pltpu.make_async_copy(gain_hbm, gain_ref, sems.at[0])]
    for i in range(5):
        rows = pl.ds(i * 144, 144)
        copies.append(pltpu.make_async_copy(tok_hbm.at[rows], tok_ref.at[rows], sems.at[1 + i]))
    copies.append(pltpu.make_async_copy(w_hbm, w_ref, sems.at[6]))
    for copy in copies:
        copy.start()
    copies[0].wait()
    for r in range(0, TOK, 144):
        copies[1 + r // 144].wait()
        rows = tok_ref[r : r + 144, :].astype(F32)
        normed[r : r + 144, :] = norm_rows(rows, gain_ref[...].reshape(1, D)).astype(BF)
    normed[TOK:PAD, :] = jnp.zeros((PAD - TOK, D), BF)
    copies[6].wait()
    for s in range(4):
        for p in range(3):
            src = pl.multiple_of(p * 192 + (y ^ s) * HD, 16)
            wp[s * 144 + p * HD : s * 144 + (p + 1) * HD, :] = w_ref[pl.ds(src, HD), :]
    for j in range(0, PAD, 256):
        res = lax.dot_general(
            wp[...], normed[j : j + 256, :], (((1,), (1,)), ((), ())), preferred_element_type=F32
        )
        for s in range(4):
            for p in range(3):
                part = res[s * 144 + p * HD : s * 144 + (p + 1) * HD]
                if p == 0:
                    part = part * (LOG2E / HD**0.5)
                slabs[s][p, :, j : j + 256] = part.astype(BF)
    for (first, _, rows), base in zip(CHUNKS, bases):
        start = first + slot * rows
        short = start + rows > TOK

        @pl.when(jnp.logical_not(short))
        def _(start=start, rows=rows, base=base):
            base[...] = tok_ref[pl.ds(pl.multiple_of(start, 16), rows), :]

        @pl.when(short)
        def _(first=first, rows=rows, base=base):
            kept = max(0, TOK - (first + 7 * rows))
            base[...] = jnp.zeros((rows, D), BF)
            if kept < rows:
                base[0:kept, :] = tok_ref[TOK - kept : TOK, :]


def attend_kernel(at_ref, *refs, lo, cols, sets, first, last):
    refs = list(refs)
    slabs = [refs.pop(0) for _ in range(4)]
    kvs = refs.pop(0) if sets else None
    carry = None if first else [refs.pop(0) for _ in range(2)]
    outs = [refs.pop(0) for _ in range(4 if last else 2)]
    keys, vals, qs, kmax = refs[:4]
    final = refs[4] if last else None
    blocks = 4 * max(1, len(sets))
    off = lo if carry is not None and carry[0].shape[-1] == ALL else 0

    most = jnp.zeros((1, TOK), F32)
    for b in range(blocks):
        pair = kvs.at[sets[b // 4], b % 4] if sets else slabs[b].at[1:3]
        kt = pair[0, :, :TOK].astype(F32)
        most = jnp.maximum(most, jnp.sum(kt * kt, axis=0, keepdims=True))
        keys[b] = kt.T.astype(BF)
        vals[b, :HD, :] = pair[1, :, :TOK]
        vals[b, HD:, :] = jnp.ones((16, TOK), BF)
    kmax[0] = jnp.max(most)
    for start, width, _ in CHUNKS:
        for s in range(4):
            at = 4 * start + s * width - lo
            if 0 <= at < cols:
                qs[:, at : at + width] = slabs[s][0, :, start : start + width]

    def finish(i, j, acc, m):
        if not last:
            outs[0][:, pl.ds(j, QW)] = acc
            outs[1][:, pl.ds(j, QW)] = m
            return
        done = (acc[:HD] / acc[HD : HD + 1]).astype(BF)
        half = final.shape[-1]
        for p in range(QW // half):
            source, side = i * (QW // half // 2) + p // 2, p % 2
            final[source, at_ref[SIDE] ^ side] = done[:, p * half : (p + 1) * half]

    def tile(i, _):
        j = pl.multiple_of(i * QW, QW)
        qt = qs[:, pl.ds(j, QW)]
        qf = qt.astype(F32)
        safe = jnp.max(jnp.sum(qf * qf, axis=0, keepdims=True)) * kmax[0] <= SAFE
        if first:
            m0, acc0 = jnp.full((1, QW), -1e30, F32), jnp.zeros((64, QW), F32)
        else:
            acc0, m0 = (c[:, pl.ds(pl.multiple_of(off + j, QW), QW)] for c in carry)
            safe = jnp.logical_and(safe, jnp.max(jnp.abs(m0)) == 0.0)

        @pl.when(safe)
        def _():
            acc, scores = acc0, dot(keys[0], qt)
            for b in range(blocks):
                ahead = dot(keys[b + 1], qt) if b + 1 < blocks else None
                acc = acc + dot(vals[b], jnp.exp2(scores).astype(BF))
                scores = ahead
            finish(i, j, acc, jnp.zeros((1, QW), F32))

        @pl.when(jnp.logical_not(safe))
        def _():
            def block(b, st):
                m, acc = st
                scores = dot(keys[b], qt)
                fresh = jnp.maximum(m, jnp.max(scores, axis=0, keepdims=True))
                acc = acc * jnp.exp2(m - fresh)
                return fresh, acc + dot(vals[b], jnp.exp2(scores - fresh).astype(BF))

            m, acc = lax.fori_loop(0, blocks, block, (m0, acc0))
            finish(i, j, acc, m)

        return 0

    lax.fori_loop(0, cols // QW, tile, 0)
    if last:
        for s in range(4):
            outs[s][...] = final[s]


def attend(at, slabs, kvs, carry, lo, cols, last, sets=()):
    first = carry is None
    blocks = 4 * max(1, len(sets))
    if last:
        outs = (shape(2, HD, cols // 8),) * 4
    else:
        outs = (shape(64, cols, dtype=F32), shape(1, cols, dtype=F32))
    scratch = [
        pltpu.VMEM((blocks, TOK, HD), BF),
        pltpu.VMEM((blocks, 64, TOK), BF),
        pltpu.VMEM((HD, cols), BF),
        pltpu.SMEM((1,), F32),
    ]
    if last:
        scratch.append(pltpu.VMEM((4, 2, HD, cols // 8), BF))
    kernel = functools.partial(
        attend_kernel, lo=lo, cols=cols, sets=sets, first=first, last=last
    )
    flops = cols * blocks * TOK * 8 * HD
    return call(kernel, outs, scratch, flops, 14, n_smem=1)(
        at, *slabs, *(() if kvs is None else (kvs,)), *(carry or ())
    )


def mix_kernel(at_ref, b0, b1, b2, b3, other_ref, w_ref, wo_ref, *refs, rows):
    outs, (heads, tall, lhs) = refs[:4], refs[4:]
    y, g = at_ref[Y], at_ref[GROUP_AT]
    for i in range(2):
        for s, back in enumerate((b0, b1, b2, b3)):
            to = pl.ds(pl.multiple_of((y ^ s) * HD, 16), HD)
            heads[to, :] = other_ref[s] if i else back[0]
        tall[...] = heads[...].astype(F32).T.astype(BF)
        for s in range(4):
            src = pl.multiple_of((g ^ s) * rows, 16)
            lhs[i, s * rows : (s + 1) * rows, :] = tall[pl.ds(src, rows), :]
    for j in range(0, D, 512):
        term = dot(lhs[0], w_ref[:, j : j + 512]) + dot(lhs[1], wo_ref[:, j : j + 512])
        term = term.astype(BF)
        for s in range(4):
            outs[s][:, j : j + 512] = term[s * rows : (s + 1) * rows]


def norm_kernel(base_ref, t0, t1, t2, t3, gain_ref, mixed_ref, post_ref):
    mixed = base_ref[...].astype(F32)
    for t in (t0, t1, t2, t3):
        mixed = mixed + t[...].astype(F32)
    mixed_ref[...] = mixed
    post_ref[...] = norm_rows(mixed, gain_ref[...].reshape(1, D)).astype(BF)


def ffn_kernel(p0, p1, p2, p3, up, down, ea, eb, *refs, rows):
    outs, (posts, acc) = refs[:4], refs[4:]
    for s, p in enumerate((p0, p1, p2, p3)):
        posts[s * rows : (s + 1) * rows, :] = p[...]
    n = 384

    def hidden(u):
        return jax.nn.gelu(dot(posts[...], u), approximate=True).astype(BF)

    acc[...] = dot(hidden(up[:, :n]), down[:n, :])
    acc[...] += dot(hidden(up[:, n:]), down[n:, :])
    ha, hb = hidden(ea[:D, :]), hidden(eb[:D, :])
    for j in range(4):
        at = D + j * n
        add = dot(ha, ea[at : at + n, :]) + dot(hb, eb[at : at + n, :])
        acc[:, j * n : (j + 1) * n] += add
    for s in range(4):
        outs[s][...] = acc[s * rows : (s + 1) * rows, :].astype(BF)


def sum_kernel(mixed_ref, t0, t1, t2, t3, out_ref):
    total = mixed_ref[...]
    for t in (t0, t1, t2, t3):
        total = total + t[...].astype(F32)
    out_ref[...] = total.astype(BF)


def slot_of(t):
    zl, x = t >> 2, t & 3
    return ((x & 1) ^ (x >> 1)) * 4 + zl * 2 + (x >> 1)


def pack_kernel(at_ref, up_ref, down_ref, out_ref):
    n = out_ref.shape[1]
    at = pl.multiple_of(at_ref[CORE] * n, 128)
    out_ref[:D, :] = up_ref[:, pl.ds(at, n)]
    for j in range(4):
        out_ref[D + j * n : D + (j + 1) * n, :] = down_ref[pl.ds(at, n), j * n : (j + 1) * n]


def place_kernel(at_ref, *refs):
    o_ref, sems = refs[-2:]
    own, by1, by3, by2, by6 = refs[:5]
    first = [own.at[0], by1.at[0], by2, by3.at[0], own.at[1], by1.at[1], by6, by3.at[1]]
    pieces = (first, refs[5:13])

    def each(act):
        for c, ((begin, _, rows), slabs) in enumerate(zip(CHUNKS, pieces)):
            for s, slab in enumerate(slabs):
                start = begin + slot_of(at_ref[T] ^ s) * rows
                kept = min(rows, TOK - (begin + 7 * rows))
                short = start + rows > TOK
                sem = sems.at[c * 8 + s]

                @pl.when(jnp.logical_not(short))
                def _(slab=slab, start=start, rows=rows, sem=sem):
                    to = o_ref.at[pl.ds(pl.multiple_of(start, 16), rows)]
                    act(pltpu.make_async_copy(slab, to, sem))

                if kept < rows:

                    @pl.when(short)
                    def _(slab=slab, kept=kept, sem=sem):
                        to = o_ref.at[pl.ds(TOK - kept, kept)]
                        act(pltpu.make_async_copy(slab.at[pl.ds(0, kept)], to, sem))

    each(lambda copy: copy.start())
    each(lambda copy: copy.wait())


def per_device(tokens, norm_gain, w_qkv, w_out, post_gain, w_up, w_down):
    t = lax.axis_index(TENSOR)
    slot = slot_of(t)
    at = jnp.stack([lax.axis_index("y"), lax.axis_index("core"), slot // 4, slot, slot % 4, t])

    w = jnp.transpose(w_qkv, (1, 2, 0)).reshape(-1, D)
    outs = (shape(3, HD, PAD),) * 4 + tuple(shape(c[2], D) for c in CHUNKS)
    scratch = [
        pltpu.VMEM((PAD, D), BF),
        pltpu.VMEM((576, D), BF),
        pltpu.VMEM((TOK, D), BF),
        pltpu.VMEM((D,), F32),
        pltpu.VMEM((576, D), BF),
        pltpu.SemaphoreType.DMA((7,)),
    ]
    *slabs, base0, base1 = call(
        qkv_kernel, outs, scratch, 2 * 576 * D * PAD, 52, n_smem=1, n_any=3
    )(at, tokens, norm_gain, w)
    far = swap(slabs[2], "y", 4, 2)
    slabs = [slabs[0], swap(slabs[1], "y", 4, 1), far, swap(slabs[3], "y", 4, 3)]
    kv_own = slabs[0][1:]
    z_own = swap(kv_own, "zh", 2, 1)
    kv_rest = jnp.stack([s[1:] for s in slabs[1:]])
    z_rest = swap(kv_rest, "zh", 2, 1)

    out_a = tswap(w_out, PAIR)
    packed = call(pack_kernel, shape(2 * D, w_up.shape[1] // 2), flops=2**28, limit=16, n_smem=1)(
        at, w_up, w_down
    )
    extra_a = tswap(packed, PAIR)

    part = attend(at, slabs, None, None, 0, ALL, False)
    kvs = jnp.concatenate([kv_own[None], kv_rest, z_own[None], z_rest], 0)
    kvs = kvs.reshape(2, 4, 2, HD, PAD)
    kv_core = swap(kvs, "core", 2, 1)
    part = attend(at, slabs, kvs, part, 0, ALL, False, (1,))
    heads = [attend(at, slabs, kv_core, part, 0, 1024, True, (0, 1))]
    part = attend(at, slabs, kv_core, part, 1024, 2048, False, (0,))
    heads.append(attend(at, slabs, kv_core, part, 1024, 2048, True, (1,)))
    extra_b = swap(extra_a, "core", 2, 1)

    slabs = []
    for c, (_, cols, rows) in enumerate(CHUNKS):
        back = [heads[c][0]] + [swap(heads[c][s], "y", 4, s) for s in range(1, 4)]
        give = jnp.stack([b[1] for b in back])
        other = tswap(give, PAIR)
        four = (shape(rows, D),) * 4
        n = 4 * rows
        scratch = [pltpu.VMEM((192, n), BF), pltpu.VMEM((n, 192), BF), pltpu.VMEM((2, n, 192), BF)]
        kernel = functools.partial(mix_kernel, rows=rows)
        terms = call(kernel, four, scratch, 2 * n * 384 * D, 8, n_smem=1)(
            at, *back, other, w_out, out_a
        )
        terms = [terms[0]] + [tswap(terms[i + 1], m) for i, m in enumerate(GROUP)]
        outs = (shape(rows, D, dtype=F32), shape(rows, D))
        mixed, post = call(norm_kernel, outs, limit=6)((base0, base1)[c], *terms, post_gain)
        posts = [post] + [tswap(post, m) for m in GROUP]
        scratch = [pltpu.VMEM((n, D), BF), pltpu.VMEM((n, D), F32)]
        kernel = functools.partial(ffn_kernel, rows=rows)
        downs = call(kernel, four, scratch, 8 * n * 768 * D, 20)(
            *posts, w_up, w_down, extra_a, extra_b
        )
        downs = [downs[0]] + [tswap(downs[i + 1], m) for i, m in enumerate(GROUP)]
        final = call(sum_kernel, shape(rows, D), limit=4)(mixed, *downs)
        if c == 0:
            both = jnp.stack([final, tswap(final, 4)])
            by1, by3 = tswap(both, 1), tswap(both, 3)
            slabs = [both, by1, by3, tswap(by3[0], 1), tswap(by1[1], 3)]
        else:
            by3, by5 = tswap(final, 3), tswap(final, 5)
            by1, by7, by4 = (tswap(final, s) for s in (1, 7, 4))
            slabs += [final, by1, tswap(by3, 1), by3, by4, by5, tswap(by5, 3), by7]
    sems = [pltpu.SemaphoreType.DMA((16,))]
    return call(place_kernel, shape(TOK, D), sems, limit=12, n_smem=1, out=ANY)(at, *slabs)


def solution(mesh):
    seq, ten = ("zh", "y", "core"), TENSOR
    fine = Mesh(mesh.devices.reshape(2, 4, 2, 2, 2, 2), seq + ten)
    placed = (P(seq, None), P(), P(None, None, ten), P(ten, None), P(), P(None, ten), P(ten, None))

    return jax.shard_map(
        per_device, mesh=fine, in_specs=placed, out_specs=P(seq, None), check_vma=False
    )
```

```python
import functools

import jax
import jax.numpy as jnp
from jax import lax
from jax.experimental import pallas as pl
from jax.experimental.pallas import tpu as pltpu
from jax.sharding import Mesh
from jax.sharding import PartitionSpec as P


HD = 48
D = 1536
TOK = 720
PAD = 768
QW = 512
ALL = 4 * PAD
CHUNKS = ((0, 384, 48), (384, 384, 48))
LOG2E = 1.4426950408889634
SAFE = 90.0 * 90.0
BF = jnp.bfloat16
F32 = jnp.float32
VMEM = pl.BlockSpec(memory_space=pltpu.VMEM)
SMEM = pl.BlockSpec(memory_space=pltpu.SMEM)
ANY = pl.BlockSpec(memory_space=pltpu.HBM)
PAIR = 1
TENSOR = ("zl", "xh", "xl")
Y, CORE, SIDE, SLOT, GROUP_AT, T = range(6)
GROUP = (3, 4, 7)


def swap(x, axis, size, s):
    return lax.ppermute(x, axis, [(i, i ^ s) for i in range(size)])


def tswap(x, s):
    return swap(x, TENSOR, 8, s)


def shape(*dims, dtype=BF):
    return jax.ShapeDtypeStruct(dims, dtype)


def call(kernel, outs, scratch=(), flops=0, limit=32, n_smem=0, n_any=0, out=VMEM):
    def run(*args):
        return pl.pallas_call(
            kernel,
            out_shape=outs,
            in_specs=[SMEM] * n_smem + [ANY] * n_any + [VMEM] * (len(args) - n_smem - n_any),
            out_specs=jax.tree.map(lambda _: out, outs),
            scratch_shapes=list(scratch),
            compiler_params=pltpu.CompilerParams(vmem_limit_bytes=limit * 2**20),
            cost_estimate=pl.CostEstimate(flops=flops, transcendentals=0, bytes_accessed=2**20),
        )(*args)

    return run


def norm_rows(values, gain):
    mean = jnp.mean(values, axis=-1, keepdims=True)
    centred = values - mean
    var = jnp.mean(centred * centred, axis=-1, keepdims=True)
    return centred * lax.rsqrt(var + 1e-05) * gain


def dot(a, b):
    return jnp.dot(a, b, preferred_element_type=F32)


def qkv_kernel(at_ref, tok_hbm, gain_hbm, w_hbm, *refs):
    slabs, bases = refs[:4], refs[4:6]
    normed, wp, tok_ref, gain_ref, w_ref, sems = refs[6:]
    y, slot = at_ref[Y], at_ref[SLOT]
    copies = [pltpu.make_async_copy(gain_hbm, gain_ref, sems.at[0])]
    for i in range(5):
        rows = pl.ds(i * 144, 144)
        copies.append(pltpu.make_async_copy(tok_hbm.at[rows], tok_ref.at[rows], sems.at[1 + i]))
    copies.append(pltpu.make_async_copy(w_hbm, w_ref, sems.at[6]))
    for copy in copies:
        copy.start()
    copies[0].wait()
    for r in range(0, TOK, 144):
        copies[1 + r // 144].wait()
        rows = tok_ref[r : r + 144, :].astype(F32)
        normed[r : r + 144, :] = norm_rows(rows, gain_ref[...].reshape(1, D)).astype(BF)
    normed[TOK:PAD, :] = jnp.zeros((PAD - TOK, D), BF)
    copies[6].wait()
    for s in range(4):
        for p in range(3):
            src = pl.multiple_of(p * 192 + (y ^ s) * HD, 16)
            wp[s * 144 + p * HD : s * 144 + (p + 1) * HD, :] = w_ref[pl.ds(src, HD), :]
    for j in range(0, PAD, 256):
        res = lax.dot_general(
            wp[...], normed[j : j + 256, :], (((1,), (1,)), ((), ())), preferred_element_type=F32
        )
        for s in range(4):
            for p in range(3):
                part = res[s * 144 + p * HD : s * 144 + (p + 1) * HD]
                if p == 0:
                    part = part * (LOG2E / HD**0.5)
                slabs[s][p, :, j : j + 256] = part.astype(BF)
    for (first, _, rows), base in zip(CHUNKS, bases):
        start = first + slot * rows
        short = start + rows > TOK

        @pl.when(jnp.logical_not(short))
        def _(start=start, rows=rows, base=base):
            base[...] = tok_ref[pl.ds(pl.multiple_of(start, 16), rows), :]

        @pl.when(short)
        def _(first=first, rows=rows, base=base):
            kept = max(0, TOK - (first + 7 * rows))
            base[...] = jnp.zeros((rows, D), BF)
            if 0 < kept < rows:
                base[0:kept, :] = tok_ref[TOK - kept : TOK, :]


def attend_kernel(at_ref, *refs, lo, cols, sets, first, last):
    refs = list(refs)
    slabs = [refs.pop(0) for _ in range(4)]
    kvs = refs.pop(0) if sets else None
    carry = None if first else [refs.pop(0) for _ in range(2)]
    outs = [refs.pop(0) for _ in range(4 if last else 2)]
    keys, vals, qs, kmax = refs[:4]
    final = refs[4] if last else None
    blocks = 4 * max(1, len(sets))
    off = lo if carry is not None and carry[0].shape[-1] == ALL else 0

    most = jnp.zeros((1, TOK), F32)
    for b in range(blocks):
        pair = kvs.at[sets[b // 4], b % 4] if sets else slabs[b].at[1:3]
        kt = pair[0, :, :TOK].astype(F32)
        most = jnp.maximum(most, jnp.sum(kt * kt, axis=0, keepdims=True))
        keys[b] = kt.T.astype(BF)
        vals[b, :HD, :] = pair[1, :, :TOK]
        vals[b, HD:, :] = jnp.ones((16, TOK), BF)
    kmax[0] = jnp.max(most)
    for start, width, _ in CHUNKS:
        for s in range(4):
            at = 4 * start + s * width - lo
            if 0 <= at < cols:
                qs[:, at : at + width] = slabs[s][0, :, start : start + width]

    def finish(j, acc, m):
        if not last:
            outs[0][:, pl.ds(j, QW)] = acc
            outs[1][:, pl.ds(j, QW)] = m
            return
        final[:, pl.ds(j, QW)] = acc[:HD] / acc[HD : HD + 1]

    def tile(i, _):
        j = pl.multiple_of(i * QW, QW)
        qt = qs[:, pl.ds(j, QW)]
        qf = qt.astype(F32)
        safe = jnp.max(jnp.sum(qf * qf, axis=0, keepdims=True)) * kmax[0] <= SAFE
        if first:
            m0, acc0 = jnp.full((1, QW), -1e30, F32), jnp.zeros((64, QW), F32)
        else:
            acc0, m0 = (c[:, pl.ds(pl.multiple_of(off + j, QW), QW)] for c in carry)
            safe = jnp.logical_and(safe, jnp.max(jnp.abs(m0)) == 0.0)

        @pl.when(safe)
        def _():
            acc, scores = acc0, dot(keys[0], qt)
            for b in range(blocks):
                ahead = dot(keys[b + 1], qt) if b + 1 < blocks else None
                acc = acc + dot(vals[b], jnp.exp2(scores).astype(BF))
                scores = ahead
            finish(j, acc, jnp.zeros((1, QW), F32))

        @pl.when(jnp.logical_not(safe))
        def _():
            def block(b, st):
                m, acc = st
                scores = dot(keys[b], qt)
                fresh = jnp.maximum(m, jnp.max(scores, axis=0, keepdims=True))
                acc = acc * jnp.exp2(m - fresh)
                return fresh, acc + dot(vals[b], jnp.exp2(scores - fresh).astype(BF))

            m, acc = lax.fori_loop(0, blocks, block, (m0, acc0))
            finish(j, acc, m)

        return 0

    lax.fori_loop(0, cols // QW, tile, 0)
    if last:
        half = cols // 8
        for s in range(4):
            for h in range(2):
                at = (2 * s + h) * half
                outs[s][at_ref[SIDE] ^ h] = final[:, at : at + half].astype(BF)


def attend(at, slabs, kvs, carry, lo, cols, last, sets=()):
    first = carry is None
    blocks = 4 * max(1, len(sets))
    if last:
        outs = (shape(2, HD, cols // 8),) * 4
    else:
        outs = (shape(64, cols, dtype=F32), shape(1, cols, dtype=F32))
    scratch = [
        pltpu.VMEM((blocks, TOK, HD), BF),
        pltpu.VMEM((blocks, 64, TOK), BF),
        pltpu.VMEM((HD, cols), BF),
        pltpu.SMEM((1,), F32),
    ]
    if last:
        scratch.append(pltpu.VMEM((HD, cols), F32))
    kernel = functools.partial(
        attend_kernel, lo=lo, cols=cols, sets=sets, first=first, last=last
    )
    flops = cols * blocks * TOK * 8 * HD
    return call(kernel, outs, scratch, flops, 14, n_smem=1)(
        at, *slabs, *(() if kvs is None else (kvs,)), *(carry or ())
    )


def mix_kernel(at_ref, b0, b1, b2, b3, other_ref, w_ref, wo_ref, *refs, rows):
    outs, (heads, tall, lhs) = refs[:4], refs[4:]
    y, g = at_ref[Y], at_ref[GROUP_AT]
    for i in range(2):
        for s, back in enumerate((b0, b1, b2, b3)):
            to = pl.ds(pl.multiple_of((y ^ s) * HD, 16), HD)
            heads[to, :] = other_ref[s] if i else back[0]
        tall[...] = heads[...].astype(F32).T.astype(BF)
        for s in range(4):
            src = pl.multiple_of((g ^ s) * rows, 16)
            lhs[i, s * rows : (s + 1) * rows, :] = tall[pl.ds(src, rows), :]
    for j in range(0, D, 512):
        term = dot(lhs[0], w_ref[:, j : j + 512]) + dot(lhs[1], wo_ref[:, j : j + 512])
        term = term.astype(BF)
        for s in range(4):
            outs[s][:, j : j + 512] = term[s * rows : (s + 1) * rows]


def norm_kernel(base_ref, t0, t1, t2, t3, gain_ref, mixed_ref, post_ref):
    mixed = base_ref[...].astype(F32)
    for t in (t0, t1, t2, t3):
        mixed = mixed + t[...].astype(F32)
    mixed_ref[...] = mixed
    post_ref[...] = norm_rows(mixed, gain_ref[...].reshape(1, D)).astype(BF)


def ffn_kernel(p0, p1, p2, p3, up, down, ea, eb, *refs, rows):
    outs, (posts, acc) = refs[:4], refs[4:]
    for s, p in enumerate((p0, p1, p2, p3)):
        posts[s * rows : (s + 1) * rows, :] = p[...]
    n = 384

    def hidden(u):
        return jax.nn.gelu(dot(posts[...], u), approximate=True).astype(BF)

    acc[...] = dot(hidden(up[:, :n]), down[:n, :])
    acc[...] += dot(hidden(up[:, n:]), down[n:, :])
    ha, hb = hidden(ea[:D, :]), hidden(eb[:D, :])
    for j in range(4):
        at = D + j * n
        add = dot(ha, ea[at : at + n, :]) + dot(hb, eb[at : at + n, :])
        acc[:, j * n : (j + 1) * n] += add
    for s in range(4):
        outs[s][...] = acc[s * rows : (s + 1) * rows, :].astype(BF)


def sum_kernel(mixed_ref, t0, t1, t2, t3, out_ref):
    total = mixed_ref[...]
    for t in (t0, t1, t2, t3):
        total = total + t[...].astype(F32)
    out_ref[...] = total.astype(BF)


def slot_of(t):
    zl, x = t >> 2, t & 3
    return ((x & 1) ^ (x >> 1)) * 4 + zl * 2 + (x >> 1)


def pack_kernel(at_ref, up_ref, down_ref, out_ref):
    n = out_ref.shape[1]
    at = pl.multiple_of(at_ref[CORE] * n, 128)
    out_ref[:D, :] = up_ref[:, pl.ds(at, n)]
    for j in range(4):
        out_ref[D + j * n : D + (j + 1) * n, :] = down_ref[pl.ds(at, n), j * n : (j + 1) * n]


def place_kernel(at_ref, *refs):
    o_ref, sems = refs[-2:]
    own, by1, by3, by2, by6 = refs[:5]
    first = [own.at[0], by1.at[0], by2, by3.at[0], own.at[1], by1.at[1], by6, by3.at[1]]
    pieces = (first, refs[5:13])

    def each(act):
        for c, ((begin, _, rows), slabs) in enumerate(zip(CHUNKS, pieces)):
            for s, slab in enumerate(slabs):
                start = begin + slot_of(at_ref[T] ^ s) * rows
                kept = min(rows, TOK - (begin + 7 * rows))
                short = start + rows > TOK
                sem = sems.at[c * 8 + s]

                @pl.when(jnp.logical_not(short))
                def _(slab=slab, start=start, rows=rows, sem=sem):
                    to = o_ref.at[pl.ds(pl.multiple_of(start, 16), rows)]
                    act(pltpu.make_async_copy(slab, to, sem))

                if 0 < kept < rows:

                    @pl.when(short)
                    def _(slab=slab, kept=kept, sem=sem):
                        to = o_ref.at[pl.ds(TOK - kept, kept)]
                        act(pltpu.make_async_copy(slab.at[pl.ds(0, kept)], to, sem))

    each(lambda copy: copy.start())
    each(lambda copy: copy.wait())


def per_device(tokens, norm_gain, w_qkv, w_out, post_gain, w_up, w_down):
    t = lax.axis_index(TENSOR)
    slot = slot_of(t)
    at = jnp.stack([lax.axis_index("y"), lax.axis_index("core"), slot // 4, slot, slot % 4, t])

    w = jnp.transpose(w_qkv, (1, 2, 0)).reshape(-1, D)
    outs = (shape(3, HD, PAD),) * 4 + tuple(shape(c[2], D) for c in CHUNKS)
    scratch = [
        pltpu.VMEM((PAD, D), BF),
        pltpu.VMEM((576, D), BF),
        pltpu.VMEM((TOK, D), BF),
        pltpu.VMEM((D,), F32),
        pltpu.VMEM((576, D), BF),
        pltpu.SemaphoreType.DMA((7,)),
    ]
    *slabs, base0, base1 = call(
        qkv_kernel, outs, scratch, 2 * 576 * D * PAD, 52, n_smem=1, n_any=3
    )(at, tokens, norm_gain, w)
    far = swap(slabs[2], "y", 4, 2)
    slabs = [slabs[0], swap(slabs[1], "y", 4, 1), far, swap(slabs[3], "y", 4, 3)]
    kv_own = slabs[0][1:]
    z_own = swap(kv_own, "zh", 2, 1)
    kv_rest = jnp.stack([s[1:] for s in slabs[1:]])
    z_rest = swap(kv_rest, "zh", 2, 1)

    out_a = tswap(w_out, PAIR)
    packed = call(pack_kernel, shape(2 * D, w_up.shape[1] // 2), flops=2**28, limit=16, n_smem=1)(
        at, w_up, w_down
    )
    extra_a = tswap(packed, PAIR)

    part = attend(at, slabs, None, None, 0, ALL, False)
    kvs = jnp.concatenate([kv_own[None], kv_rest, z_own[None], z_rest], 0)
    kvs = kvs.reshape(2, 4, 2, HD, PAD)
    kv_core = swap(kvs, "core", 2, 1)
    part = attend(at, slabs, kvs, part, 0, ALL, False, (1,))
    heads = [attend(at, slabs, kv_core, part, 0, ALL // 2, True, (0, 1))]
    heads.append(attend(at, slabs, kv_core, part, ALL // 2, ALL // 2, True, (0, 1)))
    extra_b = swap(extra_a, "core", 2, 1)

    slabs = []
    for c, (_, cols, rows) in enumerate(CHUNKS):
        back = [heads[c][0]] + [swap(heads[c][s], "y", 4, s) for s in range(1, 4)]
        give = jnp.stack([b[1] for b in back])
        other = tswap(give, PAIR)
        four = (shape(rows, D),) * 4
        n = 4 * rows
        scratch = [pltpu.VMEM((192, n), BF), pltpu.VMEM((n, 192), BF), pltpu.VMEM((2, n, 192), BF)]
        kernel = functools.partial(mix_kernel, rows=rows)
        terms = call(kernel, four, scratch, 2 * n * 384 * D, 8, n_smem=1)(
            at, *back, other, w_out, out_a
        )
        terms = [terms[0]] + [tswap(terms[i + 1], m) for i, m in enumerate(GROUP)]
        outs = (shape(rows, D, dtype=F32), shape(rows, D))
        mixed, post = call(norm_kernel, outs, limit=6)((base0, base1)[c], *terms, post_gain)
        posts = [post] + [tswap(post, m) for m in GROUP]
        scratch = [pltpu.VMEM((n, D), BF), pltpu.VMEM((n, D), F32)]
        kernel = functools.partial(ffn_kernel, rows=rows)
        downs = call(kernel, four, scratch, 8 * n * 768 * D, 20)(
            *posts, w_up, w_down, extra_a, extra_b
        )
        downs = [downs[0]] + [tswap(downs[i + 1], m) for i, m in enumerate(GROUP)]
        final = call(sum_kernel, shape(rows, D), limit=4)(mixed, *downs)
        if c == 0:
            both = jnp.stack([final, tswap(final, 4)])
            by1, by3 = tswap(both, 1), tswap(both, 3)
            slabs = [both, by1, by3, tswap(by3[0], 1), tswap(by1[1], 3)]
        else:
            by3, by5 = tswap(final, 3), tswap(final, 5)
            by1, by7, by4 = (tswap(final, s) for s in (1, 7, 4))
            slabs += [final, by1, tswap(by3, 1), by3, by4, by5, tswap(by5, 3), by7]
    sems = [pltpu.SemaphoreType.DMA((16,))]
    return call(place_kernel, shape(TOK, D), sems, limit=12, n_smem=1, out=ANY)(at, *slabs)


def solution(mesh):
    seq, ten = ("zh", "y", "core"), TENSOR
    fine = Mesh(mesh.devices.reshape(2, 4, 2, 2, 2, 2), seq + ten)
    placed = (P(seq, None), P(), P(None, None, ten), P(ten, None), P(), P(None, ten), P(ten, None))

    return jax.shard_map(
        per_device, mesh=fine, in_specs=placed, out_specs=P(seq, None), check_vma=False
    )
```

```python
import functools

import jax
import jax.numpy as jnp
from jax import lax
from jax.experimental import pallas as pl
from jax.experimental.pallas import tpu as pltpu
from jax.sharding import Mesh
from jax.sharding import PartitionSpec as P


HD = 48
D = 1536
TOK = 720
PAD = 768
QW = 512
ALL = 4 * PAD
CHUNKS = ((0, 256, 32), (256, 512, 64))
LOG2E = 1.4426950408889634
SAFE = 90.0 * 90.0
BF = jnp.bfloat16
F32 = jnp.float32
VMEM = pl.BlockSpec(memory_space=pltpu.VMEM)
SMEM = pl.BlockSpec(memory_space=pltpu.SMEM)
ANY = pl.BlockSpec(memory_space=pltpu.HBM)
PAIR = 1
TENSOR = ("zl", "xh", "xl")
Y, CORE, SIDE, SLOT, GROUP_AT, T = range(6)
GROUP = (3, 4, 7)


def swap(x, axis, size, s):
    return lax.ppermute(x, axis, [(i, i ^ s) for i in range(size)])


def tswap(x, s):
    return swap(x, TENSOR, 8, s)


def shape(*dims, dtype=BF):
    return jax.ShapeDtypeStruct(dims, dtype)


def call(kernel, outs, scratch=(), flops=0, limit=32, n_smem=0, n_any=0, out=VMEM):
    def run(*args):
        return pl.pallas_call(
            kernel,
            out_shape=outs,
            in_specs=[SMEM] * n_smem + [ANY] * n_any + [VMEM] * (len(args) - n_smem - n_any),
            out_specs=jax.tree.map(lambda _: out, outs),
            scratch_shapes=list(scratch),
            compiler_params=pltpu.CompilerParams(vmem_limit_bytes=limit * 2**20),
            cost_estimate=pl.CostEstimate(flops=flops, transcendentals=0, bytes_accessed=2**20),
        )(*args)

    return run


def norm_rows(values, gain):
    mean = jnp.mean(values, axis=-1, keepdims=True)
    centred = values - mean
    var = jnp.mean(centred * centred, axis=-1, keepdims=True)
    return centred * lax.rsqrt(var + 1e-05) * gain


def dot(a, b):
    return jnp.dot(a, b, preferred_element_type=F32)


def qkv_kernel(at_ref, tok_hbm, gain_hbm, w_hbm, *refs):
    slabs, bases = refs[:4], refs[4:6]
    normed, wp, tok_ref, gain_ref, w_ref, sems = refs[6:]
    y, slot = at_ref[Y], at_ref[SLOT]
    copies = [pltpu.make_async_copy(gain_hbm, gain_ref, sems.at[0])]
    for i in range(5):
        rows = pl.ds(i * 144, 144)
        copies.append(pltpu.make_async_copy(tok_hbm.at[rows], tok_ref.at[rows], sems.at[1 + i]))
    copies.append(pltpu.make_async_copy(w_hbm, w_ref, sems.at[6]))
    for copy in copies:
        copy.start()
    copies[0].wait()
    for r in range(0, TOK, 144):
        copies[1 + r // 144].wait()
        rows = tok_ref[r : r + 144, :].astype(F32)
        normed[r : r + 144, :] = norm_rows(rows, gain_ref[...].reshape(1, D)).astype(BF)
    normed[TOK:PAD, :] = jnp.zeros((PAD - TOK, D), BF)
    copies[6].wait()
    for s in range(4):
        for p in range(3):
            src = pl.multiple_of(p * 192 + (y ^ s) * HD, 16)
            wp[s * 144 + p * HD : s * 144 + (p + 1) * HD, :] = w_ref[pl.ds(src, HD), :]
    for j in range(0, PAD, 256):
        res = lax.dot_general(
            wp[...], normed[j : j + 256, :], (((1,), (1,)), ((), ())), preferred_element_type=F32
        )
        for s in range(4):
            for p in range(3):
                part = res[s * 144 + p * HD : s * 144 + (p + 1) * HD]
                if p == 0:
                    part = part * (LOG2E / HD**0.5)
                slabs[s][p, :, j : j + 256] = part.astype(BF)
    for (first, _, rows), base in zip(CHUNKS, bases):
        start = first + slot * rows
        short = start + rows > TOK

        @pl.when(jnp.logical_not(short))
        def _(start=start, rows=rows, base=base):
            base[...] = tok_ref[pl.ds(pl.multiple_of(start, 16), rows), :]

        @pl.when(short)
        def _(first=first, rows=rows, base=base):
            kept = max(0, TOK - (first + 7 * rows))
            base[...] = jnp.zeros((rows, D), BF)
            if kept < rows:
                base[0:kept, :] = tok_ref[TOK - kept : TOK, :]


def attend_kernel(at_ref, *refs, lo, cols, sets, first, last):
    refs = list(refs)
    slabs = [refs.pop(0) for _ in range(4)]
    kvs = refs.pop(0) if sets else None
    carry = None if first else [refs.pop(0) for _ in range(2)]
    outs = [refs.pop(0) for _ in range(4 if last else 2)]
    keys, vals, qs, kmax = refs[:4]
    final = refs[4] if last else None
    blocks = 4 * max(1, len(sets))
    off = lo if carry is not None and carry[0].shape[-1] == ALL else 0

    most = jnp.zeros((1, TOK), F32)
    for b in range(blocks):
        pair = kvs.at[sets[b // 4], b % 4] if sets else slabs[b].at[1:3]
        kt = pair[0, :, :TOK].astype(F32)
        most = jnp.maximum(most, jnp.sum(kt * kt, axis=0, keepdims=True))
        keys[b] = kt.T.astype(BF)
        vals[b, :HD, :] = pair[1, :, :TOK]
        vals[b, HD:, :] = jnp.ones((16, TOK), BF)
    kmax[0] = jnp.max(most)
    for start, width, _ in CHUNKS:
        for s in range(4):
            at = 4 * start + s * width - lo
            if 0 <= at < cols:
                qs[:, at : at + width] = slabs[s][0, :, start : start + width]

    def finish(i, j, acc, m):
        if not last:
            outs[0][:, pl.ds(j, QW)] = acc
            outs[1][:, pl.ds(j, QW)] = m
            return
        done = (acc[:HD] / acc[HD : HD + 1]).astype(BF)
        half = final.shape[-1]
        for p in range(QW // half):
            source, side = i * (QW // half // 2) + p // 2, p % 2
            final[source, at_ref[SIDE] ^ side] = done[:, p * half : (p + 1) * half]

    def tile(i, _):
        j = pl.multiple_of(i * QW, QW)
        qt = qs[:, pl.ds(j, QW)]
        qf = qt.astype(F32)
        safe = jnp.max(jnp.sum(qf * qf, axis=0, keepdims=True)) * kmax[0] <= SAFE
        if first:
            m0, acc0 = jnp.full((1, QW), -1e30, F32), jnp.zeros((64, QW), F32)
        else:
            acc0, m0 = (c[:, pl.ds(pl.multiple_of(off + j, QW), QW)] for c in carry)
            safe = jnp.logical_and(safe, jnp.max(jnp.abs(m0)) == 0.0)

        @pl.when(safe)
        def _():
            acc, scores = acc0, dot(keys[0], qt)
            for b in range(blocks):
                ahead = dot(keys[b + 1], qt) if b + 1 < blocks else None
                acc = acc + dot(vals[b], jnp.exp2(scores).astype(BF))
                scores = ahead
            finish(i, j, acc, jnp.zeros((1, QW), F32))

        @pl.when(jnp.logical_not(safe))
        def _():
            def block(b, st):
                m, acc = st
                scores = dot(keys[b], qt)
                fresh = jnp.maximum(m, jnp.max(scores, axis=0, keepdims=True))
                acc = acc * jnp.exp2(m - fresh)
                return fresh, acc + dot(vals[b], jnp.exp2(scores - fresh).astype(BF))

            m, acc = lax.fori_loop(0, blocks, block, (m0, acc0))
            finish(i, j, acc, m)

        return 0

    lax.fori_loop(0, cols // QW, tile, 0)
    if last:
        for s in range(4):
            outs[s][...] = final[s]


def attend(at, slabs, kvs, carry, lo, cols, last, sets=()):
    first = carry is None
    blocks = 4 * max(1, len(sets))
    if last:
        outs = (shape(2, HD, cols // 8),) * 4
    else:
        outs = (shape(64, cols, dtype=F32), shape(1, cols, dtype=F32))
    scratch = [
        pltpu.VMEM((blocks, TOK, HD), BF),
        pltpu.VMEM((blocks, 64, TOK), BF),
        pltpu.VMEM((HD, cols), BF),
        pltpu.SMEM((1,), F32),
    ]
    if last:
        scratch.append(pltpu.VMEM((4, 2, HD, cols // 8), BF))
    kernel = functools.partial(
        attend_kernel, lo=lo, cols=cols, sets=sets, first=first, last=last
    )
    flops = cols * blocks * TOK * 8 * HD
    return call(kernel, outs, scratch, flops, 14, n_smem=1)(
        at, *slabs, *(() if kvs is None else (kvs,)), *(carry or ())
    )


def mix_kernel(at_ref, b0, b1, b2, b3, other_ref, w_ref, wo_ref, *refs, rows):
    outs, (heads, tall, lhs) = refs[:4], refs[4:]
    y, g = at_ref[Y], at_ref[GROUP_AT]
    for i in range(2):
        for s, back in enumerate((b0, b1, b2, b3)):
            to = pl.ds(pl.multiple_of((y ^ s) * HD, 16), HD)
            heads[to, :] = other_ref[s] if i else back[0]
        tall[...] = heads[...].astype(F32).T.astype(BF)
        for s in range(4):
            src = pl.multiple_of((g ^ s) * rows, 16)
            lhs[i, s * rows : (s + 1) * rows, :] = tall[pl.ds(src, rows), :]
    for j in range(0, D, 512):
        term = dot(lhs[0], w_ref[:, j : j + 512]) + dot(lhs[1], wo_ref[:, j : j + 512])
        term = term.astype(BF)
        for s in range(4):
            outs[s][:, j : j + 512] = term[s * rows : (s + 1) * rows]


def norm_kernel(base_ref, t0, t1, t2, t3, gain_ref, mixed_ref, post_ref):
    mixed = base_ref[...].astype(F32)
    for t in (t0, t1, t2, t3):
        mixed = mixed + t[...].astype(F32)
    mixed_ref[...] = mixed
    post_ref[...] = norm_rows(mixed, gain_ref[...].reshape(1, D)).astype(BF)


def ffn_kernel(p0, p1, p2, p3, up, down, ea, eb, *refs, rows):
    outs, (posts, acc) = refs[:4], refs[4:]
    for s, p in enumerate((p0, p1, p2, p3)):
        posts[s * rows : (s + 1) * rows, :] = p[...]
    n = 384

    def hidden(u):
        return jax.nn.gelu(dot(posts[...], u), approximate=True).astype(BF)

    acc[...] = dot(hidden(up[:, :n]), down[:n, :])
    acc[...] += dot(hidden(up[:, n:]), down[n:, :])
    ha, hb = hidden(ea[:D, :]), hidden(eb[:D, :])
    for j in range(4):
        at = D + j * n
        add = dot(ha, ea[at : at + n, :]) + dot(hb, eb[at : at + n, :])
        acc[:, j * n : (j + 1) * n] += add
    for s in range(4):
        outs[s][...] = acc[s * rows : (s + 1) * rows, :].astype(BF)


def sum_kernel(mixed_ref, t0, t1, t2, t3, out_ref):
    total = mixed_ref[...]
    for t in (t0, t1, t2, t3):
        total = total + t[...].astype(F32)
    out_ref[...] = total.astype(BF)


def slot_of(t):
    zl, x = t >> 2, t & 3
    return ((x & 1) ^ (x >> 1)) * 4 + zl * 2 + (x >> 1)


def pack_kernel(at_ref, up_ref, down_ref, out_ref):
    n = out_ref.shape[1]
    at = pl.multiple_of(at_ref[CORE] * n, 128)
    out_ref[:D, :] = up_ref[:, pl.ds(at, n)]
    for j in range(4):
        out_ref[D + j * n : D + (j + 1) * n, :] = down_ref[pl.ds(at, n), j * n : (j + 1) * n]


def place_kernel(at_ref, *refs):
    o_ref, sems = refs[-2:]
    first = [refs[s % 4].at[s // 4] for s in range(8)]
    pieces = (first, refs[4:12])

    def each(act):
        for c, ((begin, _, rows), slabs) in enumerate(zip(CHUNKS, pieces)):
            for s, slab in enumerate(slabs):
                start = begin + slot_of(at_ref[T] ^ s) * rows
                kept = min(rows, TOK - (begin + 7 * rows))
                short = start + rows > TOK
                sem = sems.at[c * 8 + s]

                @pl.when(jnp.logical_not(short))
                def _(slab=slab, start=start, rows=rows, sem=sem):
                    to = o_ref.at[pl.ds(pl.multiple_of(start, 16), rows)]
                    act(pltpu.make_async_copy(slab, to, sem))

                if kept < rows:

                    @pl.when(short)
                    def _(slab=slab, kept=kept, sem=sem):
                        to = o_ref.at[pl.ds(TOK - kept, kept)]
                        act(pltpu.make_async_copy(slab.at[pl.ds(0, kept)], to, sem))

    each(lambda copy: copy.start())
    each(lambda copy: copy.wait())


def per_device(tokens, norm_gain, w_qkv, w_out, post_gain, w_up, w_down):
    t = lax.axis_index(TENSOR)
    slot = slot_of(t)
    at = jnp.stack([lax.axis_index("y"), lax.axis_index("core"), slot // 4, slot, slot % 4, t])

    w = jnp.transpose(w_qkv, (1, 2, 0)).reshape(-1, D)
    outs = (shape(3, HD, PAD),) * 4 + tuple(shape(c[2], D) for c in CHUNKS)
    scratch = [
        pltpu.VMEM((PAD, D), BF),
        pltpu.VMEM((576, D), BF),
        pltpu.VMEM((TOK, D), BF),
        pltpu.VMEM((D,), F32),
        pltpu.VMEM((576, D), BF),
        pltpu.SemaphoreType.DMA((7,)),
    ]
    *slabs, base0, base1 = call(
        qkv_kernel, outs, scratch, 2 * 576 * D * PAD, 52, n_smem=1, n_any=3
    )(at, tokens, norm_gain, w)
    far = swap(slabs[2], "y", 4, 2)
    slabs = [slabs[0], swap(slabs[1], "y", 4, 1), far, swap(slabs[3], "y", 4, 3)]
    kv_own = slabs[0][1:]
    z_own = swap(kv_own, "zh", 2, 1)
    kv_rest = jnp.stack([s[1:] for s in slabs[1:]])
    z_rest = swap(kv_rest, "zh", 2, 1)

    out_a = tswap(w_out, PAIR)
    packed = call(pack_kernel, shape(2 * D, w_up.shape[1] // 2), flops=2**28, limit=16, n_smem=1)(
        at, w_up, w_down
    )
    extra_a = tswap(packed, PAIR)

    part = attend(at, slabs, None, None, 0, ALL, False)
    kvs = jnp.concatenate([kv_own[None], kv_rest, z_own[None], z_rest], 0)
    kvs = kvs.reshape(2, 4, 2, HD, PAD)
    kv_core = swap(kvs, "core", 2, 1)
    part = attend(at, slabs, kvs, part, 0, ALL, False, (1,))
    heads = [attend(at, slabs, kv_core, part, 0, 1024, True, (0, 1))]
    heads.append(attend(at, slabs, kv_core, part, 1024, 2048, True, (0, 1)))
    extra_b = swap(extra_a, "core", 2, 1)

    slabs = []
    for c, (_, cols, rows) in enumerate(CHUNKS):
        back = [heads[c][0]] + [swap(heads[c][s], "y", 4, s) for s in range(1, 4)]
        give = jnp.stack([b[1] for b in back])
        other = tswap(give, PAIR)
        four = (shape(rows, D),) * 4
        n = 4 * rows
        scratch = [pltpu.VMEM((192, n), BF), pltpu.VMEM((n, 192), BF), pltpu.VMEM((2, n, 192), BF)]
        kernel = functools.partial(mix_kernel, rows=rows)
        terms = call(kernel, four, scratch, 2 * n * 384 * D, 8, n_smem=1)(
            at, *back, other, w_out, out_a
        )
        terms = [terms[0]] + [tswap(terms[i + 1], m) for i, m in enumerate(GROUP)]
        outs = (shape(rows, D, dtype=F32), shape(rows, D))
        mixed, post = call(norm_kernel, outs, limit=6)((base0, base1)[c], *terms, post_gain)
        posts = [post] + [tswap(post, m) for m in GROUP]
        scratch = [pltpu.VMEM((n, D), BF), pltpu.VMEM((n, D), F32)]
        kernel = functools.partial(ffn_kernel, rows=rows)
        downs = call(kernel, four, scratch, 8 * n * 768 * D, 20)(
            *posts, w_up, w_down, extra_a, extra_b
        )
        downs = [downs[0]] + [tswap(downs[i + 1], m) for i, m in enumerate(GROUP)]
        final = call(sum_kernel, shape(rows, D), limit=4)(mixed, *downs)
        if c == 0:
            both = jnp.stack([final, tswap(final, 4)])
            slabs = [both] + [tswap(both, s) for s in (1, 2, 3)]
        else:
            by3, by5 = tswap(final, 3), tswap(final, 5)
            by1, by7, by4 = (tswap(final, s) for s in (1, 7, 4))
            slabs += [final, by1, tswap(by3, 1), by3, by4, by5, tswap(by5, 3), by7]
    sems = [pltpu.SemaphoreType.DMA((16,))]
    return call(place_kernel, shape(TOK, D), sems, limit=12, n_smem=1, out=ANY)(at, *slabs)


def solution(mesh):
    seq, ten = ("zh", "y", "core"), TENSOR
    fine = Mesh(mesh.devices.reshape(2, 4, 2, 2, 2, 2), seq + ten)
    placed = (P(seq, None), P(), P(None, None, ten), P(ten, None), P(), P(None, ten), P(ten, None))

    return jax.shard_map(
        per_device, mesh=fine, in_specs=placed, out_specs=P(seq, None), check_vma=False
    )
```

```python
import functools

import jax
import jax.numpy as jnp
from jax import lax
from jax.experimental import pallas as pl
from jax.experimental.pallas import tpu as pltpu
from jax.sharding import Mesh
from jax.sharding import PartitionSpec as P


HD = 48
D = 1536
TOK = 720
PAD = 768
QW = 512
ALL = 4 * PAD
CHUNKS = ((0, 256, 32), (256, 512, 64))
LOG2E = 1.4426950408889634
SAFE = 90.0 * 90.0
BF = jnp.bfloat16
F32 = jnp.float32
VMEM = pl.BlockSpec(memory_space=pltpu.VMEM)
SMEM = pl.BlockSpec(memory_space=pltpu.SMEM)
ANY = pl.BlockSpec(memory_space=pltpu.HBM)
PAIR = 1
TENSOR = ("zl", "xh", "xl")
Y, CORE, SIDE, SLOT, GROUP_AT, T = range(6)
GROUP = (3, 4, 7)


def swap(x, axis, size, s):
    return lax.ppermute(x, axis, [(i, i ^ s) for i in range(size)])


def tswap(x, s):
    return swap(x, TENSOR, 8, s)


def shape(*dims, dtype=BF):
    return jax.ShapeDtypeStruct(dims, dtype)


def call(kernel, outs, scratch=(), flops=0, limit=32, n_smem=0, n_any=0, out=VMEM):
    def run(*args):
        return pl.pallas_call(
            kernel,
            out_shape=outs,
            in_specs=[SMEM] * n_smem + [ANY] * n_any + [VMEM] * (len(args) - n_smem - n_any),
            out_specs=jax.tree.map(lambda _: out, outs),
            scratch_shapes=list(scratch),
            compiler_params=pltpu.CompilerParams(vmem_limit_bytes=limit * 2**20),
            cost_estimate=pl.CostEstimate(flops=flops, transcendentals=0, bytes_accessed=2**20),
        )(*args)

    return run


def norm_rows(values, gain):
    mean = jnp.mean(values, axis=-1, keepdims=True)
    centred = values - mean
    var = jnp.mean(centred * centred, axis=-1, keepdims=True)
    return centred * lax.rsqrt(var + 1e-05) * gain


def dot(a, b):
    return jnp.dot(a, b, preferred_element_type=F32)


def qkv_kernel(at_ref, tok_hbm, gain_hbm, w_hbm, *refs):
    slabs, bases = refs[:4], refs[4:6]
    normed, wp, tok_ref, gain_ref, w_ref, sems = refs[6:]
    y, slot = at_ref[Y], at_ref[SLOT]
    copies = [pltpu.make_async_copy(gain_hbm, gain_ref, sems.at[0])]
    for i in range(5):
        rows = pl.ds(i * 144, 144)
        copies.append(pltpu.make_async_copy(tok_hbm.at[rows], tok_ref.at[rows], sems.at[1 + i]))
    copies.append(pltpu.make_async_copy(w_hbm, w_ref, sems.at[6]))
    for copy in copies:
        copy.start()
    copies[0].wait()
    for r in range(0, TOK, 144):
        copies[1 + r // 144].wait()
        rows = tok_ref[r : r + 144, :].astype(F32)
        normed[r : r + 144, :] = norm_rows(rows, gain_ref[...].reshape(1, D)).astype(BF)
    normed[TOK:PAD, :] = jnp.zeros((PAD - TOK, D), BF)
    copies[6].wait()
    for s in range(4):
        for p in range(3):
            src = pl.multiple_of(p * 192 + (y ^ s) * HD, 16)
            wp[s * 144 + p * HD : s * 144 + (p + 1) * HD, :] = w_ref[pl.ds(src, HD), :]
    for j in range(0, PAD, 256):
        res = lax.dot_general(
            wp[...], normed[j : j + 256, :], (((1,), (1,)), ((), ())), preferred_element_type=F32
        )
        for s in range(4):
            for p in range(3):
                part = res[s * 144 + p * HD : s * 144 + (p + 1) * HD]
                if p == 0:
                    part = part * (LOG2E / HD**0.5)
                slabs[s][p, :, j : j + 256] = part.astype(BF)
    for (first, _, rows), base in zip(CHUNKS, bases):
        start = first + slot * rows
        short = start + rows > TOK

        @pl.when(jnp.logical_not(short))
        def _(start=start, rows=rows, base=base):
            base[...] = tok_ref[pl.ds(pl.multiple_of(start, 16), rows), :]

        @pl.when(short)
        def _(first=first, rows=rows, base=base):
            kept = max(0, TOK - (first + 7 * rows))
            base[...] = jnp.zeros((rows, D), BF)
            if kept < rows:
                base[0:kept, :] = tok_ref[TOK - kept : TOK, :]


def attend_kernel(at_ref, *refs, lo, cols, sets, first, last):
    refs = list(refs)
    slabs = [refs.pop(0) for _ in range(4)]
    kvs = refs.pop(0) if sets else None
    carry = None if first else [refs.pop(0) for _ in range(2)]
    outs = [refs.pop(0) for _ in range(4 if last else 2)]
    keys, vals, qs, kmax = refs[:4]
    final = refs[4] if last else None
    blocks = 4 * max(1, len(sets))
    off = lo if carry is not None and carry[0].shape[-1] == ALL else 0

    most = jnp.zeros((1, TOK), F32)
    for b in range(blocks):
        pair = kvs.at[sets[b // 4], b % 4] if sets else slabs[b].at[1:3]
        kt = pair[0, :, :TOK].astype(F32)
        most = jnp.maximum(most, jnp.sum(kt * kt, axis=0, keepdims=True))
        keys[b] = kt.T.astype(BF)
        vals[b, :HD, :] = pair[1, :, :TOK]
        vals[b, HD:, :] = jnp.ones((16, TOK), BF)
    kmax[0] = jnp.max(most)
    for start, width, _ in CHUNKS:
        for s in range(4):
            at = 4 * start + s * width - lo
            if 0 <= at < cols:
                qs[:, at : at + width] = slabs[s][0, :, start : start + width]

    def finish(i, j, acc, m):
        if not last:
            outs[0][:, pl.ds(j, QW)] = acc
            outs[1][:, pl.ds(j, QW)] = m
            return
        done = (acc[:HD] / acc[HD : HD + 1]).astype(BF)
        half = final.shape[-1]
        for p in range(QW // half):
            source, side = i * (QW // half // 2) + p // 2, p % 2
            final[source, at_ref[SIDE] ^ side] = done[:, p * half : (p + 1) * half]

    def tile(i, _):
        j = pl.multiple_of(i * QW, QW)
        qt = qs[:, pl.ds(j, QW)]
        qf = qt.astype(F32)
        safe = jnp.max(jnp.sum(qf * qf, axis=0, keepdims=True)) * kmax[0] <= SAFE
        if first:
            m0, acc0 = jnp.full((1, QW), -1e30, F32), jnp.zeros((64, QW), F32)
        else:
            acc0, m0 = (c[:, pl.ds(pl.multiple_of(off + j, QW), QW)] for c in carry)
            safe = jnp.logical_and(safe, jnp.max(jnp.abs(m0)) == 0.0)

        @pl.when(safe)
        def _():
            acc, scores = acc0, dot(keys[0], qt)
            for b in range(blocks):
                ahead = dot(keys[b + 1], qt) if b + 1 < blocks else None
                acc = acc + dot(vals[b], jnp.exp2(scores).astype(BF))
                scores = ahead
            finish(i, j, acc, jnp.zeros((1, QW), F32))

        @pl.when(jnp.logical_not(safe))
        def _():
            def block(b, st):
                m, acc = st
                scores = dot(keys[b], qt)
                fresh = jnp.maximum(m, jnp.max(scores, axis=0, keepdims=True))
                acc = acc * jnp.exp2(m - fresh)
                return fresh, acc + dot(vals[b], jnp.exp2(scores - fresh).astype(BF))

            m, acc = lax.fori_loop(0, blocks, block, (m0, acc0))
            finish(i, j, acc, m)

        return 0

    lax.fori_loop(0, cols // QW, tile, 0)
    if last:
        for s in range(4):
            outs[s][...] = final[s]


def attend(at, slabs, kvs, carry, lo, cols, last, sets=()):
    first = carry is None
    blocks = 4 * max(1, len(sets))
    if last:
        outs = (shape(2, HD, cols // 8),) * 4
    else:
        outs = (shape(64, cols, dtype=F32), shape(1, cols, dtype=F32))
    scratch = [
        pltpu.VMEM((blocks, TOK, HD), BF),
        pltpu.VMEM((blocks, 64, TOK), BF),
        pltpu.VMEM((HD, cols), BF),
        pltpu.SMEM((1,), F32),
    ]
    if last:
        scratch.append(pltpu.VMEM((4, 2, HD, cols // 8), BF))
    kernel = functools.partial(
        attend_kernel, lo=lo, cols=cols, sets=sets, first=first, last=last
    )
    flops = cols * blocks * TOK * 8 * HD
    return call(kernel, outs, scratch, flops, 14, n_smem=1)(
        at, *slabs, *(() if kvs is None else (kvs,)), *(carry or ())
    )


def mix_kernel(at_ref, b0, b1, b2, b3, other_ref, w_ref, wo_ref, *refs, rows):
    outs, (heads, tall, lhs) = refs[:4], refs[4:]
    y, g = at_ref[Y], at_ref[GROUP_AT]
    for i in range(2):
        for s, back in enumerate((b0, b1, b2, b3)):
            to = pl.ds(pl.multiple_of((y ^ s) * HD, 16), HD)
            heads[to, :] = other_ref[s] if i else back[0]
        tall[...] = heads[...].astype(F32).T.astype(BF)
        for s in range(4):
            src = pl.multiple_of((g ^ s) * rows, 16)
            lhs[i, s * rows : (s + 1) * rows, :] = tall[pl.ds(src, rows), :]
    for j in range(0, D, 512):
        term = dot(lhs[0], w_ref[:, j : j + 512]) + dot(lhs[1], wo_ref[:, j : j + 512])
        term = term.astype(BF)
        for s in range(4):
            outs[s][:, j : j + 512] = term[s * rows : (s + 1) * rows]


def norm_kernel(base_ref, t0, t1, t2, t3, gain_ref, mixed_ref, post_ref):
    mixed = base_ref[...].astype(F32)
    for t in (t0, t1, t2, t3):
        mixed = mixed + t[...].astype(F32)
    mixed_ref[...] = mixed
    post_ref[...] = norm_rows(mixed, gain_ref[...].reshape(1, D)).astype(BF)


def ffn_kernel(p0, p1, p2, p3, up, down, ea, eb, *refs, rows):
    outs, (posts, acc) = refs[:4], refs[4:]
    for s, p in enumerate((p0, p1, p2, p3)):
        posts[s * rows : (s + 1) * rows, :] = p[...]
    n = 384

    def hidden(u):
        return jax.nn.gelu(dot(posts[...], u), approximate=True).astype(BF)

    acc[...] = dot(hidden(up[:, :n]), down[:n, :])
    acc[...] += dot(hidden(up[:, n:]), down[n:, :])
    ha, hb = hidden(ea[:D, :]), hidden(eb[:D, :])
    for j in range(4):
        at = D + j * n
        add = dot(ha, ea[at : at + n, :]) + dot(hb, eb[at : at + n, :])
        acc[:, j * n : (j + 1) * n] += add
    for s in range(4):
        outs[s][...] = acc[s * rows : (s + 1) * rows, :].astype(BF)


def sum_kernel(mixed_ref, t0, t1, t2, t3, out_ref):
    total = mixed_ref[...]
    for t in (t0, t1, t2, t3):
        total = total + t[...].astype(F32)
    out_ref[...] = total.astype(BF)


def slot_of(t):
    zl, x = t >> 2, t & 3
    return ((x & 1) ^ (x >> 1)) * 4 + zl * 2 + (x >> 1)


def pack_kernel(at_ref, up_ref, down_ref, out_ref):
    n = out_ref.shape[1]
    at = pl.multiple_of(at_ref[CORE] * n, 128)
    out_ref[:D, :] = up_ref[:, pl.ds(at, n)]
    for j in range(4):
        out_ref[D + j * n : D + (j + 1) * n, :] = down_ref[pl.ds(at, n), j * n : (j + 1) * n]


def place_kernel(at_ref, *refs):
    o_ref, sems = refs[-2:]
    own, by1, by3, by2, by6 = refs[:5]
    first = [own.at[0], by1.at[0], by2, by3.at[0], own.at[1], by1.at[1], by6, by3.at[1]]
    pieces = (first, refs[5:13])

    def each(act):
        for c, ((begin, _, rows), slabs) in enumerate(zip(CHUNKS, pieces)):
            for s, slab in enumerate(slabs):
                start = begin + slot_of(at_ref[T] ^ s) * rows
                kept = min(rows, TOK - (begin + 7 * rows))
                short = start + rows > TOK
                sem = sems.at[c * 8 + s]

                @pl.when(jnp.logical_not(short))
                def _(slab=slab, start=start, rows=rows, sem=sem):
                    to = o_ref.at[pl.ds(pl.multiple_of(start, 16), rows)]
                    act(pltpu.make_async_copy(slab, to, sem))

                if kept < rows:

                    @pl.when(short)
                    def _(slab=slab, kept=kept, sem=sem):
                        to = o_ref.at[pl.ds(TOK - kept, kept)]
                        act(pltpu.make_async_copy(slab.at[pl.ds(0, kept)], to, sem))

    each(lambda copy: copy.start())
    each(lambda copy: copy.wait())


def per_device(tokens, norm_gain, w_qkv, w_out, post_gain, w_up, w_down):
    t = lax.axis_index(TENSOR)
    slot = slot_of(t)
    at = jnp.stack([lax.axis_index("y"), lax.axis_index("core"), slot // 4, slot, slot % 4, t])

    w = jnp.transpose(w_qkv, (1, 2, 0)).reshape(-1, D)
    outs = (shape(3, HD, PAD),) * 4 + tuple(shape(c[2], D) for c in CHUNKS)
    scratch = [
        pltpu.VMEM((PAD, D), BF),
        pltpu.VMEM((576, D), BF),
        pltpu.VMEM((TOK, D), BF),
        pltpu.VMEM((D,), F32),
        pltpu.VMEM((576, D), BF),
        pltpu.SemaphoreType.DMA((7,)),
    ]
    *slabs, base0, base1 = call(
        qkv_kernel, outs, scratch, 2 * 576 * D * PAD, 52, n_smem=1, n_any=3
    )(at, tokens, norm_gain, w)
    far = swap(slabs[2], "y", 4, 2)
    slabs = [slabs[0], swap(slabs[1], "y", 4, 1), far, swap(slabs[3], "y", 4, 3)]
    kv_own = slabs[0][1:]
    z_own = swap(kv_own, "zh", 2, 1)
    kv_rest = jnp.stack([s[1:] for s in slabs[1:]])
    z_rest = swap(kv_rest, "zh", 2, 1)

    out_a = tswap(w_out, PAIR)
    packed = call(pack_kernel, shape(2 * D, w_up.shape[1] // 2), flops=2**28, limit=16, n_smem=1)(
        at, w_up, w_down
    )
    extra_a = tswap(packed, PAIR)

    part = attend(at, slabs, None, None, 0, ALL, False)
    kvs = jnp.concatenate([kv_own[None], kv_rest, z_own[None], z_rest], 0)
    kvs = kvs.reshape(2, 4, 2, HD, PAD)
    kv_core = swap(kvs, "core", 2, 1)
    part = attend(at, slabs, kvs, part, 0, ALL, False, (1,))
    heads = [attend(at, slabs, kv_core, part, 0, 1024, True, (0, 1))]
    heads.append(attend(at, slabs, kv_core, part, 1024, 2048, True, (0, 1)))
    extra_b = swap(extra_a, "core", 2, 1)

    slabs = []
    for c, (_, cols, rows) in enumerate(CHUNKS):
        back = [heads[c][0]] + [swap(heads[c][s], "y", 4, s) for s in range(1, 4)]
        give = jnp.stack([b[1] for b in back])
        other = tswap(give, PAIR)
        four = (shape(rows, D),) * 4
        n = 4 * rows
        scratch = [pltpu.VMEM((192, n), BF), pltpu.VMEM((n, 192), BF), pltpu.VMEM((2, n, 192), BF)]
        kernel = functools.partial(mix_kernel, rows=rows)
        terms = call(kernel, four, scratch, 2 * n * 384 * D, 8, n_smem=1)(
            at, *back, other, w_out, out_a
        )
        terms = [terms[0]] + [tswap(terms[i], GROUP[i - 1]) for i in (3, 2, 1)]
        outs = (shape(rows, D, dtype=F32), shape(rows, D))
        mixed, post = call(norm_kernel, outs, limit=6)((base0, base1)[c], *terms, post_gain)
        posts = [post] + [tswap(post, m) for m in GROUP]
        scratch = [pltpu.VMEM((n, D), BF), pltpu.VMEM((n, D), F32)]
        kernel = functools.partial(ffn_kernel, rows=rows)
        downs = call(kernel, four, scratch, 8 * n * 768 * D, 20)(
            *posts, w_up, w_down, extra_a, extra_b
        )
        downs = [downs[0]] + [tswap(downs[i], GROUP[i - 1]) for i in (3, 2, 1)]
        final = call(sum_kernel, shape(rows, D), limit=4)(mixed, *downs)
        if c == 0:
            both = jnp.stack([final, tswap(final, 4)])
            by1, by3 = tswap(both, 1), tswap(both, 3)
            slabs = [both, by1, by3, tswap(by3[0], 1), tswap(by1[1], 3)]
        else:
            by3, by5 = tswap(final, 3), tswap(final, 5)
            by1, by7, by4 = (tswap(final, s) for s in (1, 7, 4))
            slabs += [final, by1, tswap(by3, 1), by3, by4, by5, tswap(by5, 3), by7]
    sems = [pltpu.SemaphoreType.DMA((16,))]
    return call(place_kernel, shape(TOK, D), sems, limit=12, n_smem=1, out=ANY)(at, *slabs)


def solution(mesh):
    seq, ten = ("zh", "y", "core"), TENSOR
    fine = Mesh(mesh.devices.reshape(2, 4, 2, 2, 2, 2), seq + ten)
    placed = (P(seq, None), P(), P(None, None, ten), P(ten, None), P(), P(None, ten), P(ten, None))

    return jax.shard_map(
        per_device, mesh=fine, in_specs=placed, out_specs=P(seq, None), check_vma=False
    )
```
